512 devices in a mesh: grp: 2 (over x_hi), lon: 16 (over y, core), lat: 16 (over z, x_lo).
Axes of the slice: x: 4 (x_hi: 2, x_lo: 2; x = x_hi * 2 + x_lo), y: 8, z: 8, core: 2. Of those that a mesh axis runs over, the one named last changes fastest.
Arguments:
- fields: bfloat16 [6, 2, 192, 192, 512], P('grp', None, 'lat', 'lon'), may hold values from -6 to 6
- surface_mask: int32 [2, 192, 192], P(None, 'lat', 'lon'), may hold values 0 or 1
- w_qkv: bfloat16 [512, 1536], replicated, may hold values from -0.25 to 0.25
- w_out: bfloat16 [512, 512], replicated, may hold values from -0.25 to 0.25
- logit_scale: float32 [8], replicated, may hold values from 2 to 12
- mask_bias: float32 [8], replicated, may hold values from -2 to 2
- w_up: bfloat16 [512, 2048], replicated, may hold values from -0.25 to 0.25
- w_down: bfloat16 [2048, 512], replicated, may hold values from -0.125 to 0.125
Outputs:
- joined: bfloat16 [6, 2, 192, 192, 512], P('grp', None, 'lat', 'lon')
The draws below stay inside these ranges and needn't reach their ends.
All inputs are finite; a program needn't handle non-finite values. No bound on the sum of `surface_mask` on one device may be relied on, other than what follows from the above.
Results may differ from the reference program's by a relative error of at most 0.006.
Values may be sent and summed in bfloat16 or wider, within the bound.
No kernel may reach another device: no remote copies, remote signals or barrier semaphores. Data moves between devices by JAX's collectives and lax.ppermute only.
A program may use at most 128 MiB of HBM per device.

```python
import math
import jax
import jax.numpy as jnp
from jax import lax

G = 6
LEV = 2
C = 512
HEADS = 8
HIDDEN_SIZE = 2048
WLAT = 6
WLON = 12
SH_LAT = 3
SH_LON = 6
NLAT = 192
NLON = 192


def plant(array, rng, least, largest):
    index_at = [jax.random.randint(jax.random.fold_in(rng, axis), (), 0, length) for axis, length in enumerate(array.shape)]
    main_axis = array.shape.index(max(array.shape))
    neighbour = index_at[:main_axis] + [(index_at[main_axis] + 1) % array.shape[main_axis]] + index_at[main_axis + 1:]
    return array.at[tuple(index_at)].set(least).at[tuple(neighbour)].set(largest)


def level_of(key, extent, pieces, least, largest):
    loudness = 1.0
    for position, shards_of in pieces:
        heights = jax.random.uniform(jax.random.fold_in(jax.random.fold_in(key, 6), position), (shards_of,), jnp.float32, least / len(pieces), largest / len(pieces))
        loudness = loudness * jnp.repeat(jnp.exp(heights), extent[position] // shards_of).reshape((-1,) + (1,) * (len(extent) - 1 - position))
    return loudness


def bell_draw(key, shape, deviation, limit, split=(), kind=jnp.bfloat16):
    array = jax.random.normal(key, shape, jnp.float32) * deviation
    if len(split) > 0:
        array = level_of(key, shape, split, -0.22, 0.18) * array
    return jnp.clip(array, min=-limit, max=limit).astype(kind)


def setup_inputs(seed: int = 0) -> dict:
    seeds = jax.random.split(jax.random.key(seed), 9)
    fields = bell_draw(seeds[0], (G, LEV, NLAT, NLON, C), 1.0, 6.0, ((0, 2), (2, 16), (3, 16)))
    surface_mask = plant((jax.random.randint(seeds[1], (LEV, NLAT, NLON), 0, 2) < 1).astype(jnp.int32), jax.random.fold_in(seeds[1], 1), 0, 1)
    w_qkv = bell_draw(seeds[2], (C, 3 * C), C ** -0.5, 0.25)
    w_out = bell_draw(seeds[3], (C, C), C ** -0.5, 0.25)
    logit_scale = jnp.clip(jnp.exp(jax.random.uniform(seeds[4], (HEADS,), jnp.float32, math.log(2.0), math.log(12.0))), 2.0, 12.0)
    mask_bias = jnp.clip(jax.random.uniform(seeds[5], (HEADS,), jnp.float32, -2.0, 2.0), -2.0, 2.0)
    w_up = bell_draw(seeds[6], (C, HIDDEN_SIZE), C ** -0.5, 0.25)
    w_down = bell_draw(seeds[7], (HIDDEN_SIZE, C), HIDDEN_SIZE ** -0.5, 0.125)
    return {"fields": fields, "surface_mask": surface_mask, "w_qkv": w_qkv, "w_out": w_out, "logit_scale": logit_scale, "mask_bias": mask_bias, "w_up": w_up, "w_down": w_down}


def layer_norm(values):
    centred = values - lax.optimization_barrier(jnp.mean(values, -1, keepdims=True))
    return centred * lax.rsqrt(lax.optimization_barrier(jnp.mean(centred * centred, -1, keepdims=True)) + 1e-05)

def unit_heads(mixed_part, head_count):
    shaped = mixed_part.reshape(mixed_part.shape[0], head_count, -1)
    scaled = shaped * lax.rsqrt(lax.optimization_barrier(jnp.mean(shaped * shaped, -1, keepdims=True)) + 1e-06)
    return scaled.reshape(mixed_part.shape).astype(jnp.bfloat16)

def windowed(tensor, nlat, nlon):
    lead = tensor.shape[:2]
    rest = tensor.shape[4:]
    shaped = tensor.reshape(lead + (nlat // WLAT, WLAT, nlon // WLON, WLON) + rest)
    order = (2, 4, 0, 1, 3, 5) + tuple(range(6, 6 + len(rest)))
    moved = jnp.transpose(shaped, order)
    return moved.reshape((nlat // WLAT * (nlon // WLON), lead[0] * lead[1] * WLAT * WLON) + rest)

def attend_window(window_args, scale, head_count):
    query_win, key_win, value_win, bias_win, region_win = window_args
    tokens, model_width = query_win.shape
    head_size = model_width // head_count
    query_heads = query_win.astype(jnp.float32).reshape(tokens, head_count, head_size)
    key_heads = key_win.astype(jnp.float32).reshape(tokens, head_count, head_size)
    value_heads = value_win.astype(jnp.float32).reshape(tokens, head_count, head_size)
    scores = jnp.einsum('qhd,khd->hqk', query_heads, key_heads)
    scores = scores * (scale / head_size)[:, None, None] + bias_win[:, None, :]
    same_region = region_win[:, None] == region_win[None, :]
    weights = jnp.where(same_region[None], jnp.exp(scores), 0.0).astype(jnp.bfloat16)
    weights = lax.optimization_barrier(weights).astype(jnp.float32)
    totals = lax.optimization_barrier(jnp.sum(weights, -1))
    weighted = jnp.einsum('hqk,khd->qhd', weights, value_heads)
    ratio = weighted / jnp.transpose(totals)[:, :, None]
    return ratio.astype(jnp.bfloat16).reshape(tokens, model_width)

def reference(fields, surface_mask, w_qkv, w_out, logit_scale, mask_bias, w_up, w_down):
    groups, levels, nlat, nlon, model_width = fields.shape
    head_count = logit_scale.shape[0]
    rolled = jnp.roll(fields, (-SH_LAT, -SH_LON), axis=(2, 3))
    marks = jnp.roll(surface_mask, (-SH_LAT, -SH_LON), axis=(1, 2)).astype(jnp.float32)
    normed = layer_norm(rolled.astype(jnp.float32)).astype(jnp.bfloat16)
    mixed = jnp.dot(normed.reshape(-1, model_width), w_qkv, preferred_element_type=jnp.float32)
    grid_shape = (groups, levels, nlat, nlon, model_width)
    queries = unit_heads(mixed[:, :model_width], head_count).reshape(grid_shape)
    key_part = unit_heads(mixed[:, model_width:2 * model_width], head_count).reshape(grid_shape)
    value_part = mixed[:, 2 * model_width:].astype(jnp.bfloat16).reshape(grid_shape)
    window_count = nlat // WLAT * (nlon // WLON)
    key_bias = mask_bias[:, None, None, None] * marks[None]
    key_bias = key_bias.reshape(head_count, levels, nlat // WLAT, WLAT, nlon // WLON, WLON)
    key_bias = jnp.transpose(key_bias, (2, 4, 0, 1, 3, 5)).reshape(window_count, head_count, -1)
    key_bias = jnp.tile(key_bias, (1, 1, groups))
    row_ids = jnp.arange(nlat, dtype=jnp.int32)
    flag_rows = (row_ids >= nlat - SH_LAT).astype(jnp.int32)
    flag_grid = jnp.broadcast_to(flag_rows[None, None, :, None], (1, levels, nlat, nlon))
    region_win = jnp.tile(windowed(flag_grid, nlat, nlon), (1, groups))

    def attend_block(window_args):
        return attend_window(window_args, logit_scale, head_count)
    attended = lax.map(attend_block, (windowed(queries, nlat, nlon), windowed(key_part, nlat, nlon), windowed(value_part, nlat, nlon), key_bias, region_win))
    attended = attended.reshape(nlat // WLAT, nlon // WLON, groups, levels, WLAT, WLON, model_width)
    attended = jnp.transpose(attended, (2, 3, 0, 4, 1, 5, 6)).reshape(grid_shape)
    projected = jnp.dot(attended.reshape(-1, model_width), w_out, preferred_element_type=jnp.float32)
    projected = projected.astype(jnp.bfloat16).reshape(grid_shape)
    unrolled = jnp.roll(projected, (SH_LAT, SH_LON), axis=(2, 3))
    residual = (fields.astype(jnp.float32) + unrolled.astype(jnp.float32)).astype(jnp.bfloat16)
    mlp_in = layer_norm(residual.astype(jnp.float32)).astype(jnp.bfloat16)
    hidden = jax.nn.gelu(jnp.dot(mlp_in.reshape(-1, model_width), w_up, preferred_element_type=jnp.float32), approximate=True).astype(jnp.bfloat16)
    update = jnp.dot(hidden, w_down, preferred_element_type=jnp.float32).reshape(grid_shape)
    return (residual.astype(jnp.float32) + update).astype(jnp.bfloat16)
```

```python
import functools

import jax
import jax.numpy as jnp
from jax import lax
from jax.experimental import pallas as pl
from jax.experimental.pallas import tpu as pltpu
from jax.sharding import PartitionSpec as P

LANES = 128
SH_LAT = 3
SH_LON = 6
WLAT = 6
LOG2E = 1.4426950408889634
EXCLUDED = -1e30
VMEM = pl.BlockSpec(memory_space=pltpu.VMEM)
SMEM = pl.BlockSpec(memory_space=pltpu.SMEM)


def to_pairs(fields):
    groups, levels, lat_rows, lon_cells, width = fields.shape
    cells = jnp.transpose(fields, (0, 2, 3, 1, 4))
    cells = cells.reshape(groups, lat_rows, lon_cells, levels, width // LANES, LANES)
    cells = jnp.transpose(cells, (0, 1, 2, 4, 3, 5))
    return cells.reshape(groups, lat_rows, lon_cells, levels * (width // LANES), LANES)


def from_pairs(cells, levels):
    groups, lat_rows, lon_cells, rows, lanes = cells.shape
    cells = cells.reshape(groups, lat_rows, lon_cells, rows // levels, levels, lanes)
    cells = jnp.transpose(cells, (0, 1, 2, 4, 3, 5))
    cells = cells.reshape(groups, lat_rows, lon_cells, levels, (rows // levels) * lanes)
    return jnp.transpose(cells, (0, 3, 1, 2, 4))


def shifted(array, axes, by):
    if isinstance(axes, str):
        count = lax.axis_size(axes)
        return lax.ppermute(array, axes, [(i, (i + by) % count) for i in range(count)])
    outer, inner = (lax.axis_size(axis) for axis in axes)
    pairs = [
        (i * inner + j, ((i + by) % outer) * inner + (j + by) % inner)
        for i in range(outer)
        for j in range(inner)
    ]
    return lax.ppermute(array, axes, pairs)


def cells_to_tokens(pieces, cells_scr, tokens_scr, row):
    count = 0
    for piece in pieces:
        size = piece.shape[0]
        cells_scr[count * 8 : (count + size) * 8, :] = piece.reshape(size * 8, LANES).astype(
            jnp.float32
        )
        count += size
    for level in range(2):
        for tile in range(4):
            tokens_scr[tile, row + level * count : row + (level + 1) * count, :] = cells_scr[
                pl.ds(2 * tile + level, count, stride=8), :
            ]


def tokens_to_cells(tokens_scr, row, count, cells_scr):
    for level in range(2):
        for tile in range(4):
            cells_scr[pl.ds(2 * tile + level, count, stride=8), :] = tokens_scr[
                tile, row + level * count : row + (level + 1) * count, :
            ]


def whole_rows(tokens_scr):
    return jnp.concatenate([tokens_scr[tile] for tile in range(4)], axis=1)


def layer_norm(values):
    centred = values - jnp.mean(values, -1, keepdims=True)
    return centred * lax.rsqrt(jnp.mean(centred * centred, -1, keepdims=True) + 1e-05)


def head_squares(values, head_size):
    width = 256
    rows = lax.broadcasted_iota(jnp.int32, (width, width), 0) // head_size
    cols = lax.broadcasted_iota(jnp.int32, (width, width), 1) // head_size
    averaging = jnp.where(rows == cols, 1.0 / head_size, 0.0).astype(jnp.bfloat16)
    squares = (values * values).astype(jnp.bfloat16)
    return jnp.concatenate(
        [
            jnp.dot(
                squares[:, at : at + width], averaging, preferred_element_type=jnp.float32
            )
            for at in range(0, values.shape[1], width)
        ],
        axis=1,
    )


def unit_heads(values, head_size):
    return values * lax.rsqrt(head_squares(values, head_size) + 1e-06)


def load_window_cells(own, east, south, corner, cells_scr, tokens_scr):
    cells_to_tokens([own[0:108]], cells_scr, tokens_scr, 0)
    cells_to_tokens([east[0:108]], cells_scr, tokens_scr, 216)
    cells_to_tokens([own[108:162], east[108:162]], cells_scr, tokens_scr, 432)
    cells_to_tokens([south[0:54], corner[0:54]], cells_scr, tokens_scr, 648)


def attend(query_ref, key_ref, value_ref, rows_ref, bias_ref, head_size, store):
    half = rows_ref.shape[1]
    lane = lax.broadcasted_iota(jnp.int32, (half, LANES), 1)

    def one(step, carry):
        window = step // 4
        pair = step % 4
        base = pl.multiple_of(window * half, 16)
        at = pl.multiple_of(pair * LANES, LANES)
        queries = query_ref[pl.ds(base, half), pl.ds(at, LANES)]
        keys = key_ref[pl.ds(base, half), pl.ds(at, LANES)]
        values = value_ref[pl.ds(base, half), pl.ds(at, LANES)]
        marks = rows_ref[pl.ds(window, 1), :]
        first = rows_ref[pl.ds(2 + window, 1), :]
        second = rows_ref[pl.ds(4 + window, 1), :]
        total = None
        for side in range(2):
            mine = (lane < head_size) if side == 0 else (lane >= head_size)
            scores = lax.dot_general(
                queries,
                jnp.where(mine, keys, jnp.zeros_like(keys)),
                (((1,), (1,)), ((), ())),
                preferred_element_type=jnp.float32,
            )
            bias = marks * bias_ref[2 * pair + side]
            scores = jnp.concatenate(
                [scores[: half // 2] + (bias + first), scores[half // 2 :] + (bias + second)], 0
            )
            weights = jnp.exp2(scores).astype(jnp.bfloat16)
            operand = jnp.concatenate(
                [
                    jnp.where(mine, values, jnp.zeros_like(values)),
                    jnp.where(mine, 1.0, 0.0).astype(jnp.bfloat16),
                ],
                axis=1,
            )
            part = jnp.dot(weights, operand, preferred_element_type=jnp.float32)
            total = part if total is None else total + part
        store(window, pair, base, at, total)
        return carry

    lax.fori_loop(0, 8, one, 0)


def own_kernel(
    head_size,
    own,
    east,
    south,
    corner,
    w_qkv,
    scale,
    rows_ref,
    bias_ref,
    query_out,
    total_out,
    cells_scr,
    tokens_scr,
    key_scr,
    value_scr,
):
    load_window_cells(own, east, south, corner, cells_scr, tokens_scr)
    width = w_qkv.shape[0]
    normed = layer_norm(whole_rows(tokens_scr)).astype(jnp.bfloat16)
    mixed = jnp.dot(normed, w_qkv[:, :width], preferred_element_type=jnp.float32)
    query_out[...] = (unit_heads(mixed, head_size) * scale[...]).astype(jnp.bfloat16)
    mixed = jnp.dot(normed, w_qkv[:, width : 2 * width], preferred_element_type=jnp.float32)
    key_scr[...] = unit_heads(mixed, head_size).astype(jnp.bfloat16)
    value_scr[...] = jnp.dot(
        normed, w_qkv[:, 2 * width :], preferred_element_type=jnp.float32
    ).astype(jnp.bfloat16)

    def store(window, pair, base, at, total):
        total_out[pair, pl.ds(base, total.shape[0]), :] = total

    attend(query_out, key_scr, value_scr, rows_ref, bias_ref, head_size, store)


def partner_kernel(
    head_size,
    own,
    rest,
    query_ref,
    total_in,
    w_kv,
    w_out,
    rows_ref,
    bias_ref,
    own_out,
    east_out,
    south_out,
    corner_out,
    cells_scr,
    tokens_scr,
    key_scr,
    value_scr,
    attended_scr,
):
    load_window_cells(
        own, rest.at[0:162], rest.at[162:216], rest.at[216:270], cells_scr, tokens_scr
    )
    width = w_kv.shape[0]
    normed = layer_norm(whole_rows(tokens_scr)).astype(jnp.bfloat16)
    mixed = jnp.dot(normed, w_kv[:, width : 2 * width], preferred_element_type=jnp.float32)
    key_scr[...] = unit_heads(mixed, head_size).astype(jnp.bfloat16)
    value_scr[...] = jnp.dot(
        normed, w_kv[:, 2 * width :], preferred_element_type=jnp.float32
    ).astype(jnp.bfloat16)

    def store(window, pair, base, at, total):
        span = pl.ds(base, total.shape[0])
        total = total + total_in[pair, span, :]
        attended_scr[span, pl.ds(at, LANES)] = (total[:, :LANES] / total[:, LANES:]).astype(
            jnp.bfloat16
        )

    attend(query_ref, key_scr, value_scr, rows_ref, bias_ref, head_size, store)
    projected = jnp.dot(attended_scr[...], w_out[...], preferred_element_type=jnp.float32)
    for tile in range(4):
        tokens_scr[tile] = projected[:, tile * LANES : (tile + 1) * LANES]

    def put(row, count, outs):
        tokens_to_cells(tokens_scr, row, count, cells_scr)
        at = 0
        for out, first, size in outs:
            out[first : first + size] = (
                cells_scr[at * 8 : (at + size) * 8, :].astype(jnp.bfloat16).reshape(size, 8, LANES)
            )
            at += size

    put(0, 108, [(own_out, 0, 108)])
    put(216, 108, [(east_out, 0, 108)])
    put(432, 108, [(own_out, 108, 54), (east_out, 108, 54)])
    put(648, 108, [(south_out, 0, 54), (corner_out, 0, 54)])


def joining_kernel(
    fields, own, west, north, corner, w_up, w_down, out, cells_scr, tokens_scr, normed_scr, chunk
):
    groups = fields.shape[0]

    def add(g, lats, lons, piece, first, shape):
        size = shape[0] * shape[1]
        term = piece[first + g * size : first + (g + 1) * size].astype(jnp.float32)
        term = term.reshape(shape + (8, LANES))
        summed = fields[g, lats[0] : lats[1], lons[0] : lons[1]].astype(jnp.float32) + term
        cells_scr[g, lats[0] : lats[1], lons[0] : lons[1]] = summed.astype(jnp.bfloat16).astype(
            jnp.float32
        )

    for g in range(groups):
        for lons, big, small in (((6, 12), own, north), ((0, 6), west, corner)):
            add(g, (3, 9), lons, big, 0, (6, 6))
            add(g, (9, 12), lons, big, 108, (3, 6))
            add(g, (0, 3), lons, small, 0, (3, 6))
    cells = groups * 144
    flat = cells_scr.reshape(cells * 8, LANES)
    for level in range(2):
        for tile in range(4):
            tokens_scr[level * cells : (level + 1) * cells, tile * LANES : (tile + 1) * LANES] = (
                flat[pl.ds(2 * tile + level, cells, stride=8), :]
            )
    normed_scr[...] = layer_norm(tokens_scr[...]).astype(jnp.bfloat16)

    def one(step, carry):
        span = pl.ds(pl.multiple_of(step * chunk, 16), chunk)
        hidden = jnp.dot(normed_scr[span, :], w_up[...], preferred_element_type=jnp.float32)
        hidden = jax.nn.gelu(hidden, approximate=True).astype(jnp.bfloat16)
        tokens_scr[span, :] = tokens_scr[span, :] + jnp.dot(
            hidden, w_down[...], preferred_element_type=jnp.float32
        )
        return carry

    lax.fori_loop(0, 2 * cells // chunk, one, 0)
    for level in range(2):
        for tile in range(4):
            flat[pl.ds(2 * tile + level, cells, stride=8), :] = tokens_scr[
                level * cells : (level + 1) * cells, tile * LANES : (tile + 1) * LANES
            ]
    out[...] = cells_scr[...].astype(jnp.bfloat16)


def mark_rows(own, east, south, corner, groups, last_band):
    def part(marks, lats, lons):
        block = marks[:, lats[0] : lats[1], lons[0] : lons[1]].reshape(2, 1, -1)
        return jnp.broadcast_to(block, (2, groups, block.shape[2])).reshape(2, -1)

    upper = jnp.concatenate(
        [part(own, (3, 9), (6, 12)).reshape(-1), part(east, (3, 9), (0, 6)).reshape(-1)]
    )
    lower = jnp.concatenate(
        [
            jnp.concatenate([part(own, (9, 12), (6, 12)), part(east, (9, 12), (0, 6))], 1).reshape(-1),
            jnp.concatenate([part(south, (0, 3), (6, 12)), part(corner, (0, 3), (0, 6))], 1).reshape(-1),
        ]
    )
    keys = upper.shape[0]
    later = jnp.arange(keys) >= keys // 2
    none = jnp.zeros((keys,), jnp.float32)
    out_first = jnp.where(last_band & later, EXCLUDED, 0.0)
    out_second = jnp.where(last_band & ~later, EXCLUDED, 0.0)
    return jnp.stack([upper, lower, none, out_first, none, out_second, none, none])


def per_device(fields, surface_mask, w_qkv, w_out, logit_scale, mask_bias, w_up, w_down):
    groups, levels, lat_rows, lon_cells, width = fields.shape
    heads = logit_scale.shape[0]
    head_size = width // heads
    tokens = groups * levels * lat_rows * lon_cells
    cells = to_pairs(fields)
    tile = (8, LANES)
    flags = surface_mask.reshape(-1).astype(jnp.bfloat16)
    flags = jnp.pad(flags, (0, 8 * LANES - flags.shape[0])).reshape((1,) + tile)

    def piece(lats, lons):
        return cells[:, lats[0] : lats[1], lons[0] : lons[1]].reshape((-1,) + tile)

    own = jnp.concatenate([piece((3, 9), (6, 12)), piece((9, 12), (6, 12))])
    east = jnp.concatenate([piece((3, 9), (0, 6)), piece((9, 12), (0, 6)), flags])
    south = jnp.concatenate([piece((0, 3), (6, 12)), flags])
    corner = jnp.concatenate([piece((0, 3), (0, 6)), flags])
    east = shifted(east, "lon", -1)
    south = shifted(south, "lat", -1)
    corner = shifted(corner, ("lon", "lat"), -1)
    own_across = shifted(own, "grp", 1)
    rest_across = shifted(jnp.concatenate([east[:162], south[:54], corner[:54]]), "grp", 1)

    def marks_of(received):
        flat = received.reshape(-1)[: levels * lat_rows * lon_cells].astype(jnp.float32)
        return flat.reshape(levels, lat_rows, lon_cells)

    last_band = lax.axis_index("lat") == lax.axis_size("lat") - 1
    rows = mark_rows(
        surface_mask.astype(jnp.float32),
        marks_of(east[162]),
        marks_of(south[54]),
        marks_of(corner[54]),
        groups,
        last_band,
    )
    scale = jnp.repeat(logit_scale * (LOG2E / head_size), head_size)[None]
    bias = mask_bias * LOG2E
    half_cells = groups * lat_rows * lon_cells // 4
    scratch = [
        pltpu.VMEM((half_cells * 8, LANES), jnp.float32),
        pltpu.VMEM((4, tokens, LANES), jnp.float32),
        pltpu.VMEM((tokens, width), jnp.bfloat16),
        pltpu.VMEM((tokens, width), jnp.bfloat16),
    ]
    queries, totals = pl.pallas_call(
        functools.partial(own_kernel, head_size),
        name="own",
        out_shape=(
            jax.ShapeDtypeStruct((tokens, width), jnp.bfloat16),
            jax.ShapeDtypeStruct((4, tokens, 2 * LANES), jnp.float32),
        ),
        in_specs=[VMEM] * 7 + [SMEM],
        out_specs=(VMEM, VMEM),
        scratch_shapes=scratch,
        cost_estimate=pl.CostEstimate(
            flops=6 * 10**9, bytes_accessed=8 * 10**6, transcendentals=3 * 10**6
        ),
    )(own, east, south, corner, w_qkv, scale, rows, bias)
    shapes = [jax.ShapeDtypeStruct((n,) + tile, jnp.bfloat16) for n in (162, 162, 54, 54)]
    own, east, south, corner = pl.pallas_call(
        functools.partial(partner_kernel, head_size),
        name="partner",
        out_shape=shapes,
        in_specs=[VMEM] * 7 + [SMEM],
        out_specs=[VMEM] * 4,
        scratch_shapes=scratch + [pltpu.VMEM((tokens, width), jnp.bfloat16)],
        cost_estimate=pl.CostEstimate(
            flops=6 * 10**9, bytes_accessed=8 * 10**6, transcendentals=3 * 10**6
        ),
    )(own_across, rest_across, queries, totals, w_qkv, w_out, rows, bias)
    east = shifted(east, "lon", 1)
    south = shifted(south, "lat", 1)
    corner = shifted(corner, ("lon", "lat"), 1)
    joined = pl.pallas_call(
        functools.partial(joining_kernel, chunk=288),
        name="joining",
        out_shape=jax.ShapeDtypeStruct(cells.shape, jnp.bfloat16),
        in_specs=[VMEM] * 7,
        out_specs=VMEM,
        scratch_shapes=[
            pltpu.VMEM(cells.shape, jnp.float32),
            pltpu.VMEM((tokens, width), jnp.float32),
            pltpu.VMEM((tokens, width), jnp.bfloat16),
        ],
        cost_estimate=pl.CostEstimate(
            flops=4 * 10**9, bytes_accessed=8 * 10**6, transcendentals=2 * 10**6
        ),
    )(cells, own, east, south, corner, w_up, w_down)
    return from_pairs(joined, levels)


def solution(mesh):
    return jax.shard_map(
        per_device,
        mesh=mesh,
        in_specs=(
            P("grp", None, "lat", "lon", None),
            P(None, "lat", "lon"),
            P(),
            P(),
            P(),
            P(),
            P(),
            P(),
        ),
        out_specs=P("grp", None, "lat", "lon", None),
        check_vma=False,
    )
```

```python
import functools

import jax
import jax.numpy as jnp
import numpy as np
from jax import lax
from jax.experimental import pallas as pl
from jax.experimental.pallas import tpu as pltpu
from jax.sharding import PartitionSpec as P

LANES = 128
SH_LAT = 3
SH_LON = 6
WLAT = 6
LOG2E = 1.4426950408889634
EXCLUDED = -1e30
VMEM = pl.BlockSpec(memory_space=pltpu.VMEM)
SMEM = pl.BlockSpec(memory_space=pltpu.SMEM)
ROOM = pltpu.CompilerParams(vmem_limit_bytes=24 << 20)


def to_pairs(fields):
    groups, levels, lat_rows, lon_cells, width = fields.shape
    cells = jnp.transpose(fields, (0, 2, 3, 1, 4))
    cells = cells.reshape(groups, lat_rows, lon_cells, levels, width // LANES, LANES)
    cells = jnp.transpose(cells, (0, 1, 2, 4, 3, 5))
    return cells.reshape(groups, lat_rows, lon_cells, levels * (width // LANES), LANES)


def from_pairs(cells, levels):
    groups, lat_rows, lon_cells, rows, lanes = cells.shape
    cells = cells.reshape(groups, lat_rows, lon_cells, rows // levels, levels, lanes)
    cells = jnp.transpose(cells, (0, 1, 2, 4, 3, 5))
    cells = cells.reshape(groups, lat_rows, lon_cells, levels, (rows // levels) * lanes)
    return jnp.transpose(cells, (0, 3, 1, 2, 4))


def shifted(array, axes, by):
    if isinstance(axes, str):
        count = lax.axis_size(axes)
        return lax.ppermute(array, axes, [(i, (i + by) % count) for i in range(count)])
    outer, inner = (lax.axis_size(axis) for axis in axes)
    pairs = [
        (i * inner + j, ((i + by) % outer) * inner + (j + by) % inner)
        for i in range(outer)
        for j in range(inner)
    ]
    return lax.ppermute(array, axes, pairs)


def cells_to_tokens(pieces, cells_scr, tokens_scr, row):
    count = 0
    for piece in pieces:
        size = piece.shape[0]
        cells_scr[count * 8 : (count + size) * 8, :] = piece.reshape(size * 8, LANES).astype(
            jnp.float32
        )
        count += size
    for level in range(2):
        for tile in range(4):
            tokens_scr[tile, row + level * count : row + (level + 1) * count, :] = cells_scr[
                pl.ds(2 * tile + level, count, stride=8), :
            ]


def tokens_to_cells(tokens_scr, row, count, cells_scr):
    for level in range(2):
        for tile in range(4):
            cells_scr[pl.ds(2 * tile + level, count, stride=8), :] = tokens_scr[
                tile, row + level * count : row + (level + 1) * count, :
            ]


def whole_rows(tokens_scr):
    return jnp.concatenate([tokens_scr[tile] for tile in range(4)], axis=1)


def layer_norm(values):
    centred = values - jnp.mean(values, -1, keepdims=True)
    return centred * lax.rsqrt(jnp.mean(centred * centred, -1, keepdims=True) + 1e-05)


def head_squares(values, head_size):
    width = 256
    rows = lax.broadcasted_iota(jnp.int32, (width, width), 0) // head_size
    cols = lax.broadcasted_iota(jnp.int32, (width, width), 1) // head_size
    averaging = jnp.where(rows == cols, 1.0 / head_size, 0.0).astype(jnp.bfloat16)
    squares = (values * values).astype(jnp.bfloat16)
    return jnp.concatenate(
        [
            jnp.dot(
                squares[:, at : at + width], averaging, preferred_element_type=jnp.float32
            )
            for at in range(0, values.shape[1], width)
        ],
        axis=1,
    )


def unit_heads(values, head_size):
    return values * lax.rsqrt(head_squares(values, head_size) + 1e-06)


def window_columns(part):
    rows, lanes = [], []
    for source_parts in part:
        for level in range(2):
            for source, lats, lons in source_parts:
                for _ in range(3):
                    for lat in range(*lats):
                        for lon in range(*lons):
                            rows.append(24 * source + 2 * lat + level)
                            lanes.append(lon)
    keys = np.arange(len(rows))
    pick_row = np.zeros((96, len(rows)), np.float32)
    pick_row[np.array(rows), keys] = 1
    pick_lane = np.zeros((16, len(rows)), np.float32)
    pick_lane[np.array(lanes), keys] = 1
    return pick_row, pick_lane


def pack_kernel(cells, mask, own, west, north, flags, sems):
    copies = []
    for g in range(3):
        for dst, first, lats, lons in (
            (west, 0, (3, 9), (0, 6)),
            (west, 108, (9, 12), (0, 6)),
            (west, 162, (0, 3), (0, 6)),
            (own, 0, (3, 9), (6, 12)),
            (own, 108, (9, 12), (6, 12)),
            (north, 0, (0, 3), (6, 12)),
        ):
            rows = lats[1] - lats[0]
            copies.append(
                pltpu.make_async_copy(
                    cells.at[g, lats[0] : lats[1], lons[0] : lons[1]],
                    dst.at[pl.ds(first + g * rows * 6, rows * 6)].reshape(rows, 6, 8, LANES),
                    sems,
                )
            )
    for copy in copies:
        copy.start()
    flags[...] = jnp.zeros(flags.shape, jnp.float32)
    for lat in range(12):
        flags[2 * lat : 2 * lat + 2, 0:12] = mask[lat].astype(jnp.float32)
    tile = flags[...].astype(jnp.bfloat16).reshape(3, 8, LANES)
    west[216:219] = tile
    north[54:57] = tile
    for copy in copies:
        copy.wait()


def attend(query_ref, key_ref, value_ref, bias_ref, head_size, store):
    half = query_ref.shape[0]
    lane = lax.broadcasted_iota(jnp.int32, (half, LANES), 1)

    def one(pair, carry):
        at = pl.multiple_of(pair * LANES, LANES)
        queries = query_ref[:, pl.ds(at, LANES)]
        keys = key_ref[:, pl.ds(at, LANES)]
        values = value_ref[:, pl.ds(at, LANES)]
        total = None
        for side in range(2):
            mine = (lane < head_size) if side == 0 else (lane >= head_size)
            scores = lax.dot_general(
                queries,
                jnp.where(mine, keys, jnp.zeros_like(keys)),
                (((1,), (1,)), ((), ())),
                preferred_element_type=jnp.float32,
            )
            first = bias_ref[pl.ds(2 * pair + side, 1), :]
            second = bias_ref[pl.ds(8 + 2 * pair + side, 1), :]
            scores = jnp.concatenate(
                [scores[: half // 2] + first, scores[half // 2 :] + second], 0
            )
            weights = jnp.exp2(scores).astype(jnp.bfloat16)
            operand = jnp.concatenate(
                [
                    jnp.where(mine, values, jnp.zeros_like(values)),
                    jnp.where(mine, 1.0, 0.0).astype(jnp.bfloat16),
                ],
                axis=1,
            )
            part = jnp.dot(weights, operand, preferred_element_type=jnp.float32)
            total = part if total is None else total + part
        store(pair, at, total)
        return carry

    [one(p, 0) for p in range(4)]


def gather(window, own, east, south, cells_scr, tokens_scr):
    if window == 0:
        cells_to_tokens([own[0:108]], cells_scr, tokens_scr, 0)
        cells_to_tokens([east[0:108]], cells_scr, tokens_scr, 216)
    else:
        cells_to_tokens([own[108:162], east[108:162]], cells_scr, tokens_scr, 0)
        cells_to_tokens([south[0:108]], cells_scr, tokens_scr, 216)


def own_kernel(
    head_size,
    window,
    own,
    east,
    south,
    north,
    w_qkv,
    params,
    pick_row,
    pick_lane,
    query_out,
    total_out,
    bias_out,
    cells_scr,
    tokens_scr,
    key_scr,
    value_scr,
):
    gather(window, own, east, south, cells_scr, tokens_scr)
    width = w_qkv.shape[0]
    marks = [north[54:57], east[216:219]]
    if window == 1:
        marks += [south[108:111], south[111:114]]
    marks = jnp.concatenate([m.reshape(24, LANES).astype(jnp.float32) for m in marks], 0)
    spread = lax.dot_general(
        marks,
        pick_row[0 : marks.shape[0], :],
        (((0,), (0,)), ((), ())),
        preferred_element_type=jnp.float32,
    )
    marks = jnp.sum(spread[0:16] * pick_lane[...], 0, keepdims=True)
    bias = params[4:12, 0:1] * marks
    bias_out[0:8, :] = bias
    bias_out[8:16, :] = bias
    if window == 1:
        keys = marks.shape[1]
        later = lax.broadcasted_iota(jnp.int32, (8, keys), 1) >= keys // 2
        excluded = params[12:13, 0:1]
        bias_out[0:8, :] = bias + jnp.where(later, excluded, 0.0)
        bias_out[8:16, :] = bias + jnp.where(later, 0.0, excluded)
    scale = jnp.concatenate([params[i : i + 1, :] for i in range(4)], 1)
    normed = layer_norm(whole_rows(tokens_scr)).astype(jnp.bfloat16)
    mixed = jnp.dot(normed, w_qkv[:, :width], preferred_element_type=jnp.float32)
    query_out[...] = (unit_heads(mixed, head_size) * scale).astype(jnp.bfloat16)
    mixed = jnp.dot(normed, w_qkv[:, width : 2 * width], preferred_element_type=jnp.float32)
    key_scr[...] = unit_heads(mixed, head_size).astype(jnp.bfloat16)
    value_scr[...] = jnp.dot(
        normed, w_qkv[:, 2 * width :], preferred_element_type=jnp.float32
    ).astype(jnp.bfloat16)

    def store(pair, at, total):
        total_out[pair] = total

    attend(query_out, key_scr, value_scr, bias_out, head_size, store)


def partner_kernel(
    head_size,
    window,
    own,
    east,
    south,
    query_ref,
    total_in,
    bias_ref,
    w_qkv,
    w_out,
    *rest,
):
    outs, (cells_scr, tokens_scr, key_scr, value_scr, attended_scr) = rest[:-5], rest[-5:]
    gather(window, own, east, south, cells_scr, tokens_scr)
    width = w_qkv.shape[0]
    normed = layer_norm(whole_rows(tokens_scr)).astype(jnp.bfloat16)
    mixed = jnp.dot(normed, w_qkv[:, width : 2 * width], preferred_element_type=jnp.float32)
    key_scr[...] = unit_heads(mixed, head_size).astype(jnp.bfloat16)
    value_scr[...] = jnp.dot(
        normed, w_qkv[:, 2 * width :], preferred_element_type=jnp.float32
    ).astype(jnp.bfloat16)

    def store(pair, at, total):
        total = total + total_in[pair]
        attended_scr[:, pl.ds(at, LANES)] = (total[:, :LANES] / total[:, LANES:]).astype(
            jnp.bfloat16
        )

    attend(query_ref, key_scr, value_scr, bias_ref, head_size, store)
    projected = jnp.dot(attended_scr[...], w_out[...], preferred_element_type=jnp.float32)
    for tile in range(4):
        tokens_scr[tile] = projected[:, tile * LANES : (tile + 1) * LANES]

    def put(row, count, outs):
        tokens_to_cells(tokens_scr, row, count, cells_scr)
        at = 0
        for out, size in outs:
            out[...] = (
                cells_scr[at * 8 : (at + size) * 8, :].astype(jnp.bfloat16).reshape(size, 8, LANES)
            )
            at += size

    if window == 0:
        put(0, 108, [(outs[0], 108)])
        put(216, 108, [(outs[1], 108)])
    else:
        put(0, 108, [(outs[0], 54), (outs[1], 54)])
        put(216, 108, [(outs[2], 54), (outs[3], 54)])


def joining_kernel(bands, chunk, fields, w_up, w_down, *rest):
    pieces, (out, cells_scr, tokens_scr, normed_scr) = rest[: 2 * len(bands)], rest[-4:]
    groups = fields.shape[0]
    at = 0
    for band, (first, rows) in enumerate(bands):
        for g in range(groups):
            for side, lons in enumerate(((6, 12), (0, 6))):
                size = rows * 6
                term = pieces[2 * band + side][g * size : (g + 1) * size].astype(jnp.float32)
                term = term.reshape(rows, 6, 8, LANES)
                summed = fields[g, first : first + rows, lons[0] : lons[1]].astype(jnp.float32)
                summed = (summed + term).astype(jnp.bfloat16).astype(jnp.float32)
                cells_scr[g, at : at + rows, lons[0] : lons[1]] = summed
        at += rows
    cells = groups * at * 12
    flat = cells_scr.reshape(cells * 8, LANES)
    for level in range(2):
        for tile in range(4):
            tokens_scr[level * cells : (level + 1) * cells, tile * LANES : (tile + 1) * LANES] = (
                flat[pl.ds(2 * tile + level, cells, stride=8), :]
            )
    normed_scr[...] = layer_norm(tokens_scr[...]).astype(jnp.bfloat16)

    def one(step, carry):
        span = pl.ds(pl.multiple_of(step * chunk, 16), chunk)
        hidden = jnp.dot(normed_scr[span, :], w_up[...], preferred_element_type=jnp.float32)
        hidden = jax.nn.gelu(hidden, approximate=True).astype(jnp.bfloat16)
        tokens_scr[span, :] = tokens_scr[span, :] + jnp.dot(
            hidden, w_down[...], preferred_element_type=jnp.float32
        )
        return carry

    lax.fori_loop(0, 2 * cells // chunk, one, 0)
    for level in range(2):
        for tile in range(4):
            flat[pl.ds(2 * tile + level, cells, stride=8), :] = tokens_scr[
                level * cells : (level + 1) * cells, tile * LANES : (tile + 1) * LANES
            ]
    if len(bands) == 1:
        out[...] = cells_scr[...].astype(jnp.bfloat16)
        return
    done = rest[2 * len(bands)]
    at = 0
    for first, rows in bands:
        out[:, first : first + rows] = cells_scr[:, at : at + rows].astype(jnp.bfloat16)
        at += rows
    out[:, 3:9] = done[...]


def per_device(fields, surface_mask, w_qkv, w_out, logit_scale, mask_bias, w_up, w_down):
    groups, levels, lat_rows, lon_cells, width = fields.shape
    heads = logit_scale.shape[0]
    head_size = width // heads
    half = groups * levels * lat_rows * lon_cells // 2
    cells = to_pairs(fields)
    tile = (8, LANES)

    def pieces(*counts):
        return tuple(jax.ShapeDtypeStruct((n,) + tile, jnp.bfloat16) for n in counts)

    def call(kernel, name, outs, scratch, flops, arrays):
        return pl.pallas_call(
            kernel,
            name=name,
            compiler_params=ROOM,
            out_shape=outs,
            in_specs=[VMEM] * len(arrays),
            out_specs=jax.tree.map(lambda _: VMEM, outs),
            scratch_shapes=scratch,
            cost_estimate=pl.CostEstimate(
                flops=flops, bytes_accessed=4 * 10**6, transcendentals=10**6
            ),
        )(*arrays)

    own, west, north = pl.pallas_call(
        pack_kernel,
        name="pack",
        compiler_params=ROOM,
        out_shape=pieces(162, 219, 57),
        in_specs=[pl.BlockSpec(memory_space=pltpu.HBM), VMEM],
        out_specs=(VMEM, VMEM, VMEM),
        scratch_shapes=[pltpu.VMEM((24, LANES), jnp.float32), pltpu.SemaphoreType.DMA],
    )(cells, jnp.transpose(surface_mask, (1, 0, 2)))
    east = shifted(west, "lon", -1)
    own_across = shifted(own, "grp", 1)
    south = shifted(
        jnp.concatenate([north[:54], east[162:216], north[54:], east[216:]]), "lat", -1
    )
    east_across = shifted(east[:162], "grp", 1)
    south_across = shifted(south[:108], "grp", 1)

    last_band = lax.axis_index("lat") == lax.axis_size("lat") - 1
    params = jnp.concatenate(
        [
            jnp.repeat(logit_scale * (LOG2E / head_size), head_size).reshape(-1, LANES),
            jnp.broadcast_to((mask_bias * LOG2E)[:, None], (heads, LANES)),
            jnp.full((1, LANES), jnp.where(last_band, EXCLUDED, 0.0)),
        ]
    )
    layout = (
        (((0, (3, 9), (6, 12)),), ((1, (3, 9), (0, 6)),)),
        (((0, (9, 12), (6, 12)), (1, (9, 12), (0, 6))), ((2, (0, 3), (6, 12)), (3, (0, 3), (0, 6)))),
    )
    scratch = [
        pltpu.VMEM((half * 2, LANES), jnp.float32),
        pltpu.VMEM((4, half, LANES), jnp.float32),
        pltpu.VMEM((half, width), jnp.bfloat16),
        pltpu.VMEM((half, width), jnp.bfloat16),
    ]
    firsts = []
    for window in range(2):
        pick_row, pick_lane = window_columns(layout[window])
        firsts.append(
            call(
                functools.partial(own_kernel, head_size, window),
                "own",
                (
                    jax.ShapeDtypeStruct((half, width), jnp.bfloat16),
                    jax.ShapeDtypeStruct((4, half, 2 * LANES), jnp.float32),
                    jax.ShapeDtypeStruct((16, half), jnp.float32),
                ),
                scratch,
                3 * 10**9,
                (own, east, south if window else own, north, w_qkv, params, pick_row, pick_lane),
            )
        )
    scratch = scratch + [pltpu.VMEM((half, width), jnp.bfloat16)]
    upper_own, upper_east = call(
        functools.partial(partner_kernel, head_size, 0),
        "partner",
        pieces(108, 108),
        scratch,
        3 * 10**9,
        (own_across, east_across, own_across) + tuple(firsts[0]) + (w_qkv, w_out),
    )
    upper_west = shifted(upper_east, "lon", 1)
    lower_own, lower_east, lower_south, lower_corner = call(
        functools.partial(partner_kernel, head_size, 1),
        "partner",
        pieces(54, 54, 54, 54),
        scratch,
        3 * 10**9,
        (own_across, east_across, south_across) + tuple(firsts[1]) + (w_qkv, w_out),
    )
    lower_south = shifted(lower_south, "lat", 1)
    lower_corner = shifted(lower_corner, ("lon", "lat"), 1)
    lower_west = shifted(lower_east, "lon", 1)
    scratch = [
        pltpu.VMEM((groups, lat_rows // 2, lon_cells) + tile, jnp.float32),
        pltpu.VMEM((half, width), jnp.float32),
        pltpu.VMEM((half, width), jnp.bfloat16),
    ]
    upper = call(
        functools.partial(joining_kernel, ((3, 6),), 144),
        "joining",
        jax.ShapeDtypeStruct((groups, lat_rows // 2) + cells.shape[2:], jnp.bfloat16),
        scratch,
        2 * 10**9,
        (cells, w_up, w_down, upper_own, upper_west),
    )
    joined = call(
        functools.partial(joining_kernel, ((9, 3), (0, 3)), 144),
        "joining",
        jax.ShapeDtypeStruct(cells.shape, jnp.bfloat16),
        scratch,
        2 * 10**9,
        (cells, w_up, w_down, lower_own, lower_west, lower_south, lower_corner, upper),
    )
    return from_pairs(joined, levels)


def solution(mesh):
    return jax.shard_map(
        per_device,
        mesh=mesh,
        in_specs=(
            P("grp", None, "lat", "lon", None),
            P(None, "lat", "lon"),
            P(),
            P(),
            P(),
            P(),
            P(),
            P(),
        ),
        out_specs=P("grp", None, "lat", "lon", None),
        check_vma=False,
    )
```

```python
import functools

import jax
import jax.numpy as jnp
import numpy as np
from jax import lax
from jax.experimental import pallas as pl
from jax.experimental.pallas import tpu as pltpu
from jax.sharding import PartitionSpec as P


LANES = 128
LOG2E = 1.4426950408889634
EXCLUDED = -1e30
VMEM = pl.BlockSpec(memory_space=pltpu.VMEM)
SMEM = pl.BlockSpec(memory_space=pltpu.SMEM)
ROOM = pltpu.CompilerParams(vmem_limit_bytes=24 << 20)


def to_pairs(fields):
    groups, levels, lat_rows, lon_cells, width = fields.shape
    cells = jnp.transpose(fields, (0, 2, 3, 1, 4))
    cells = cells.reshape(groups, lat_rows, lon_cells, levels, width // LANES, LANES)
    cells = jnp.transpose(cells, (0, 1, 2, 4, 3, 5))
    return cells.reshape(groups, lat_rows, lon_cells, levels * (width // LANES), LANES)


def from_pairs(cells, levels):
    groups, lat_rows, lon_cells, rows, lanes = cells.shape
    cells = cells.reshape(groups, lat_rows, lon_cells, rows // levels, levels, lanes)
    cells = jnp.transpose(cells, (0, 1, 2, 4, 3, 5))
    cells = cells.reshape(groups, lat_rows, lon_cells, levels, (rows // levels) * lanes)
    return jnp.transpose(cells, (0, 3, 1, 2, 4))


def shifted(array, lon=0, lat=0, across=False):
    axes = ("grp", "lon", "lat")
    sizes = [lax.axis_size(axis) for axis in axes]

    def place(g, i, j):
        return (g * sizes[1] + i % sizes[1]) * sizes[2] + j % sizes[2]

    pairs = [
        (place(g, i, j), place(1 - g if across else g, i + lon, j + lat))
        for g in range(sizes[0])
        for i in range(sizes[1])
        for j in range(sizes[2])
    ]
    return lax.ppermute(array, axes, pairs)


def cells_to_tokens(pieces, cells_scr, tokens_scr, row):
    count = 0
    for piece in pieces:
        size = piece.shape[0]
        cells_scr[count * 8 : (count + size) * 8, :] = piece.reshape(size * 8, LANES).astype(
            jnp.float32
        )
        count += size
    for level in range(2):
        for tile in range(4):
            tokens_scr[tile, row + level * count : row + (level + 1) * count, :] = cells_scr[
                pl.ds(2 * tile + level, count, stride=8), :
            ]


def tokens_to_cells(tokens_scr, row, count, cells_scr):
    for level in range(2):
        for tile in range(4):
            cells_scr[pl.ds(2 * tile + level, count, stride=8), :] = tokens_scr[
                tile, row + level * count : row + (level + 1) * count, :
            ]


def whole_rows(tokens_scr):
    return jnp.concatenate([tokens_scr[tile] for tile in range(4)], axis=1)


def layer_norm(values):
    centred = values - jnp.mean(values, -1, keepdims=True)
    return centred * lax.rsqrt(jnp.mean(centred * centred, -1, keepdims=True) + 1e-05)


def head_squares(values, head_size):
    width = 256
    rows = lax.broadcasted_iota(jnp.int32, (width, width), 0) // head_size
    cols = lax.broadcasted_iota(jnp.int32, (width, width), 1) // head_size
    averaging = jnp.where(rows == cols, 1.0 / head_size, 0.0).astype(jnp.bfloat16)
    squares = (values * values).astype(jnp.bfloat16)
    return jnp.concatenate(
        [
            jnp.dot(
                squares[:, at : at + width], averaging, preferred_element_type=jnp.float32
            )
            for at in range(0, values.shape[1], width)
        ],
        axis=1,
    )


def unit_heads(values, head_size):
    return values * lax.rsqrt(head_squares(values, head_size) + 1e-06)


def window_columns(part):
    rows, lanes = [], []
    for source_parts in part:
        for level in range(2):
            for source, lats, lons in source_parts:
                for _ in range(3):
                    for lat in range(*lats):
                        for lon in range(*lons):
                            rows.append(24 * source + 2 * lat + level)
                            lanes.append(lon)
    keys = np.arange(len(rows))
    pick_row = np.zeros((96, len(rows)), np.float32)
    pick_row[np.array(rows), keys] = 1
    pick_lane = np.zeros((16, len(rows)), np.float32)
    pick_lane[np.array(lanes), keys] = 1
    return pick_row, pick_lane


def pack_kernel(cells, mask, own, west, north, flags, sems):
    copies = []
    for g in range(3):
        for dst, first, lats, lons in (
            (west, 0, (3, 9), (0, 6)),
            (west, 108, (9, 12), (0, 6)),
            (west, 162, (0, 3), (0, 6)),
            (own, 0, (3, 9), (6, 12)),
            (own, 108, (9, 12), (6, 12)),
            (north, 0, (0, 3), (6, 12)),
        ):
            rows = lats[1] - lats[0]
            copies.append(
                pltpu.make_async_copy(
                    cells.at[g, lats[0] : lats[1], lons[0] : lons[1]],
                    dst.at[pl.ds(first + g * rows * 6, rows * 6)].reshape(rows, 6, 8, LANES),
                    sems,
                )
            )
    for copy in copies:
        copy.start()
    flags[...] = jnp.zeros(flags.shape, jnp.float32)
    for lat in range(12):
        flags[2 * lat : 2 * lat + 2, 0:12] = mask[lat].astype(jnp.float32)
    tile = flags[...].astype(jnp.bfloat16).reshape(3, 8, LANES)
    west[216:219] = tile
    north[54:57] = tile
    for copy in copies:
        copy.wait()


def again_kernel(east, out):
    out[...] = east[0:162]


def southward_kernel(east, north, after, out):
    out[0:54] = north[0:54]
    out[54:108] = east[162:216]
    out[108:111] = north[54:57]
    out[111:114] = east[216:219]


def attend(query_ref, key_ref, value_ref, bias_ref, head_size, store):
    half = query_ref.shape[0]
    lane = lax.broadcasted_iota(jnp.int32, (half, LANES), 1)

    def one(pair, carry):
        at = pl.multiple_of(pair * LANES, LANES)
        queries = query_ref[:, pl.ds(at, LANES)]
        keys = key_ref[:, pl.ds(at, LANES)]
        values = value_ref[:, pl.ds(at, LANES)]
        total = None
        for side in range(2):
            mine = (lane < head_size) if side == 0 else (lane >= head_size)
            scores = lax.dot_general(
                queries,
                jnp.where(mine, keys, jnp.zeros_like(keys)),
                (((1,), (1,)), ((), ())),
                preferred_element_type=jnp.float32,
            )
            first = bias_ref[pl.ds(2 * pair + side, 1), :]
            second = bias_ref[pl.ds(8 + 2 * pair + side, 1), :]
            scores = jnp.concatenate(
                [scores[: half // 2] + first, scores[half // 2 :] + second], 0
            )
            weights = jnp.exp2(scores).astype(jnp.bfloat16)
            operand = jnp.concatenate(
                [
                    jnp.where(mine, values, jnp.zeros_like(values)),
                    jnp.where(mine, 1.0, 0.0).astype(jnp.bfloat16),
                ],
                axis=1,
            )
            part = jnp.dot(weights, operand, preferred_element_type=jnp.float32)
            total = part if total is None else total + part
        store(pair, at, total)
        return carry

    [one(p, 0) for p in range(4)]


def gather(window, own, east, south, cells_scr, tokens_scr):
    if window == 0:
        cells_to_tokens([own[0:108]], cells_scr, tokens_scr, 0)
        cells_to_tokens([east[0:108]], cells_scr, tokens_scr, 216)
    else:
        cells_to_tokens([own[108:162], east[108:162]], cells_scr, tokens_scr, 0)
        cells_to_tokens([south[0:108]], cells_scr, tokens_scr, 216)


def own_kernel(
    head_size,
    window,
    own,
    east,
    south,
    after,
    north,
    w_qkv,
    logit_scale,
    mask_bias,
    pick_row,
    pick_lane,
    query_out,
    total_out,
    bias_out,
    cells_scr,
    tokens_scr,
    key_scr,
    value_scr,
):
    gather(window, own, east, south, cells_scr, tokens_scr)
    width = w_qkv.shape[0]
    marks = [north[54:57], east[216:219]]
    if window == 1:
        marks += [south[108:111], south[111:114]]
    marks = jnp.concatenate([m.reshape(24, LANES).astype(jnp.float32) for m in marks], 0)
    spread = lax.dot_general(
        marks,
        pick_row[0 : marks.shape[0], :],
        (((0,), (0,)), ((), ())),
        preferred_element_type=jnp.float32,
    )
    marks = jnp.sum(spread[0:16] * pick_lane[...], 0, keepdims=True)
    heads = mask_bias.shape[1]
    rows = lax.broadcasted_iota(jnp.int32, (heads, heads), 0)
    cols = lax.broadcasted_iota(jnp.int32, (heads, heads), 1)
    column = jnp.sum(jnp.where(rows == cols, mask_bias[...], 0.0), 1, keepdims=True)
    bias = (column * LOG2E) * marks
    bias_out[0:8, :] = bias
    bias_out[8:16, :] = bias
    if window == 1:
        keys = marks.shape[1]
        later = lax.broadcasted_iota(jnp.int32, (8, keys), 1) >= keys // 2
        last = lax.axis_index("lat") == lax.axis_size("lat") - 1
        excluded = jnp.where(last, EXCLUDED, 0.0)
        bias_out[0:8, :] = bias + jnp.where(later, excluded, 0.0)
        bias_out[8:16, :] = bias + jnp.where(later, 0.0, excluded)
    head = lax.broadcasted_iota(jnp.int32, (1, width), 1) // head_size
    scale = jnp.zeros((1, width), jnp.float32)
    for i in range(heads):
        scale = jnp.where(head == i, logit_scale[0:1, i : i + 1] * (LOG2E / head_size), scale)
    normed = layer_norm(whole_rows(tokens_scr)).astype(jnp.bfloat16)
    mixed = jnp.dot(normed, w_qkv[:, :width], preferred_element_type=jnp.float32)
    query_out[...] = (unit_heads(mixed, head_size) * scale).astype(jnp.bfloat16)
    mixed = jnp.dot(normed, w_qkv[:, width : 2 * width], preferred_element_type=jnp.float32)
    key_scr[...] = unit_heads(mixed, head_size).astype(jnp.bfloat16)
    value_scr[...] = jnp.dot(
        normed, w_qkv[:, 2 * width :], preferred_element_type=jnp.float32
    ).astype(jnp.bfloat16)

    def store(pair, at, total):
        total_out[pair] = total

    attend(query_out, key_scr, value_scr, bias_out, head_size, store)


def partner_kernel(
    head_size,
    window,
    own,
    east,
    south,
    query_ref,
    total_in,
    bias_ref,
    w_qkv,
    w_out,
    *rest,
):
    outs, (cells_scr, tokens_scr, key_scr, value_scr, attended_scr) = rest[:-5], rest[-5:]
    gather(window, own, east, south, cells_scr, tokens_scr)
    width = w_qkv.shape[0]
    normed = layer_norm(whole_rows(tokens_scr)).astype(jnp.bfloat16)
    mixed = jnp.dot(normed, w_qkv[:, width : 2 * width], preferred_element_type=jnp.float32)
    key_scr[...] = unit_heads(mixed, head_size).astype(jnp.bfloat16)
    value_scr[...] = jnp.dot(
        normed, w_qkv[:, 2 * width :], preferred_element_type=jnp.float32
    ).astype(jnp.bfloat16)

    def store(pair, at, total):
        total = total + total_in[pair]
        attended_scr[:, pl.ds(at, LANES)] = (total[:, :LANES] / total[:, LANES:]).astype(
            jnp.bfloat16
        )

    attend(query_ref, key_scr, value_scr, bias_ref, head_size, store)
    projected = jnp.dot(attended_scr[...], w_out[...], preferred_element_type=jnp.float32)
    for tile in range(4):
        tokens_scr[tile] = projected[:, tile * LANES : (tile + 1) * LANES]

    def put(row, count, outs):
        tokens_to_cells(tokens_scr, row, count, cells_scr)
        at = 0
        for out, size in outs:
            out[...] = (
                cells_scr[at * 8 : (at + size) * 8, :].astype(jnp.bfloat16).reshape(size, 8, LANES)
            )
            at += size

    if window == 0:
        put(0, 108, [(outs[0], 108)])
        put(216, 108, [(outs[1], 108)])
    else:
        put(0, 108, [(outs[0], 54), (outs[1], 54)])
        put(216, 108, [(outs[2], 54), (outs[3], 54)])


def joining_kernel(bands, fields, w_up, w_down, *rest):
    pieces, (out, cells_scr, tokens_scr) = rest[: 2 * len(bands)], rest[-3:]
    if len(bands) == 2:
        out[:, 3:9] = rest[2 * len(bands)][...]
    for g in range(fields.shape[0]):
        at = 0
        for band, (first, rows) in enumerate(bands):
            for side, lons in enumerate(((6, 12), (0, 6))):
                size = rows * 6
                term = pieces[2 * band + side][g * size : (g + 1) * size].astype(jnp.float32)
                term = term.reshape(rows, 6, 8, LANES)
                summed = fields[g, first : first + rows, lons[0] : lons[1]].astype(jnp.float32)
                summed = (summed + term).astype(jnp.bfloat16).astype(jnp.float32)
                cells_scr[g, at : at + rows, lons[0] : lons[1]] = summed
            at += rows
        cells = at * 12
        flat = cells_scr.at[g].reshape(cells * 8, LANES)
        for level in range(2):
            for tile in range(4):
                tokens_scr[
                    g, level * cells : (level + 1) * cells, tile * LANES : (tile + 1) * LANES
                ] = flat[pl.ds(2 * tile + level, cells, stride=8), :]
        residual = tokens_scr[g]
        normed = layer_norm(residual).astype(jnp.bfloat16)
        hidden = jnp.dot(normed, w_up[...], preferred_element_type=jnp.float32)
        hidden = jax.nn.gelu(hidden, approximate=True).astype(jnp.bfloat16)
        joined = residual + jnp.dot(hidden, w_down[...], preferred_element_type=jnp.float32)
        for level in range(2):
            for tile in range(4):
                flat[pl.ds(2 * tile + level, cells, stride=8), :] = joined[
                    level * cells : (level + 1) * cells, tile * LANES : (tile + 1) * LANES
                ]
        if len(bands) == 1:
            out[g] = cells_scr[g].astype(jnp.bfloat16)
        else:
            at = 0
            for first, rows in bands:
                out[g, first : first + rows] = cells_scr[g, at : at + rows].astype(jnp.bfloat16)
                at += rows


def per_device(fields, surface_mask, w_qkv, w_out, logit_scale, mask_bias, w_up, w_down):
    groups, levels, lat_rows, lon_cells, width = fields.shape
    heads = logit_scale.shape[0]
    head_size = width // heads
    half = groups * levels * lat_rows * lon_cells // 2
    cells = to_pairs(fields)
    tile = (8, LANES)

    def pieces(*counts):
        return tuple(jax.ShapeDtypeStruct((n,) + tile, jnp.bfloat16) for n in counts)

    def call(kernel, outs, scratch, flops, arrays):
        return pl.pallas_call(
            kernel,
            compiler_params=ROOM,
            out_shape=outs,
            in_specs=[VMEM] * len(arrays),
            out_specs=jax.tree.map(lambda _: VMEM, outs),
            scratch_shapes=scratch,
            cost_estimate=pl.CostEstimate(
                flops=flops, bytes_accessed=4 * 10**6, transcendentals=10**6
            ),
        )(*arrays)

    own, west, north = pl.pallas_call(
        pack_kernel,
        name="pack",
        compiler_params=ROOM,
        out_shape=pieces(162, 219, 57),
        in_specs=[pl.BlockSpec(memory_space=pltpu.HBM), VMEM],
        out_specs=(VMEM, VMEM, VMEM),
        scratch_shapes=[pltpu.VMEM((24, LANES), jnp.float32), pltpu.SemaphoreType.DMA],
    )(cells, jnp.transpose(surface_mask, (1, 0, 2)))
    east = shifted(west, lon=-1)
    own_across = shifted(own, across=True)
    east_again = call(again_kernel, pieces(162)[0], [], 10**6, (east,))
    east_across = shifted(east_again, across=True)

    layout = (
        (((0, (3, 9), (6, 12)),), ((1, (3, 9), (0, 6)),)),
        (((0, (9, 12), (6, 12)), (1, (9, 12), (0, 6))), ((2, (0, 3), (6, 12)), (3, (0, 3), (0, 6)))),
    )
    scratch = [
        pltpu.VMEM((half * 2, LANES), jnp.float32),
        pltpu.VMEM((4, half, LANES), jnp.float32),
        pltpu.VMEM((half, width), jnp.bfloat16),
        pltpu.VMEM((half, width), jnp.bfloat16),
    ]
    late = scratch + [pltpu.VMEM((half, width), jnp.bfloat16)]

    def own_part(window, arrays):
        pick_row, pick_lane = window_columns(layout[window])
        return call(
            functools.partial(own_kernel, head_size, window),
            (
                jax.ShapeDtypeStruct((half, width), jnp.bfloat16),
                jax.ShapeDtypeStruct((4, half, 2 * LANES), jnp.float32),
                jax.ShapeDtypeStruct((16, half), jnp.float32),
            ),
            scratch,
            3 * 10**9,
            arrays + (w_qkv, logit_scale[None], mask_bias[None], pick_row, pick_lane),
        )

    def partner_part(window, counts, arrays, first):
        return call(
            functools.partial(partner_kernel, head_size, window),
            pieces(*counts),
            late,
            3 * 10**9,
            arrays + tuple(first) + (w_qkv, w_out),
        )

    first = own_part(0, (own, east, north, north, north))
    south = call(southward_kernel, pieces(114)[0], [], 10**6, (east, north, first[2]))
    south_across = shifted(south, lat=-1, across=True)
    south = shifted(south, lat=-1)
    upper_own, upper_east = partner_part(
        0, (108, 108), (own_across, east_across, own_across), first
    )
    upper_west = shifted(upper_east, lon=1)
    first = own_part(1, (own, east, south, upper_own, north))
    lower_own, lower_east, lower_south, lower_corner = partner_part(
        1, (54, 54, 54, 54), (own_across, east_across, south_across), first
    )
    lower_north = shifted(lower_south, lat=1)
    lower_northwest = shifted(lower_corner, lon=1, lat=1)
    lower_west = shifted(lower_east, lon=1)
    scratch = [
        pltpu.VMEM((groups, lat_rows // 2, lon_cells) + tile, jnp.float32),
        pltpu.VMEM((groups, half // groups, width), jnp.float32),
    ]
    upper = call(
        functools.partial(joining_kernel, ((3, 6),)),
        jax.ShapeDtypeStruct((groups, lat_rows // 2) + cells.shape[2:], jnp.bfloat16),
        scratch,
        2 * 10**9,
        (cells, w_up, w_down, upper_own, upper_west),
    )
    joined = call(
        functools.partial(joining_kernel, ((9, 3), (0, 3))),
        jax.ShapeDtypeStruct(cells.shape, jnp.bfloat16),
        scratch,
        2 * 10**9,
        (cells, w_up, w_down, lower_own, lower_west, lower_north, lower_northwest, upper),
    )
    return from_pairs(joined, levels)


def solution(mesh):
    return jax.shard_map(
        per_device,
        mesh=mesh,
        in_specs=(
            P("grp", None, "lat", "lon", None),
            P(None, "lat", "lon"),
            P(),
            P(),
            P(),
            P(),
            P(),
            P(),
        ),
        out_specs=P("grp", None, "lat", "lon", None),
        check_vma=False,
    )
```

```python
import functools

import jax
import jax.numpy as jnp
import numpy as np
from jax import lax
from jax.experimental import pallas as pl
from jax.experimental.pallas import tpu as pltpu
from jax.sharding import PartitionSpec as P


LANES = 128
SH_LAT = 3
LOG2E = 1.4426950408889634
EXCLUDED = -1e30
VMEM = pl.BlockSpec(memory_space=pltpu.VMEM)
SMEM = pl.BlockSpec(memory_space=pltpu.SMEM)
ROOM = pltpu.CompilerParams(vmem_limit_bytes=24 << 20)


def to_pairs(fields):
    groups, levels, lat_rows, lon_cells, width = fields.shape
    cells = jnp.transpose(fields, (0, 2, 3, 1, 4))
    cells = cells.reshape(groups, lat_rows, lon_cells, levels, width // LANES, LANES)
    cells = jnp.transpose(cells, (0, 1, 2, 4, 3, 5))
    return cells.reshape(groups, lat_rows, lon_cells, levels * (width // LANES), LANES)


def from_pairs(cells, levels):
    groups, lat_rows, lon_cells, rows, lanes = cells.shape
    cells = cells.reshape(groups, lat_rows, lon_cells, rows // levels, levels, lanes)
    cells = jnp.transpose(cells, (0, 1, 2, 4, 3, 5))
    cells = cells.reshape(groups, lat_rows, lon_cells, levels, (rows // levels) * lanes)
    return jnp.transpose(cells, (0, 3, 1, 2, 4))


def shifted(array, lon=0, lat=0, across=False):
    axes = ("grp", "lon", "lat")
    sizes = [lax.axis_size(axis) for axis in axes]

    def place(g, i, j):
        return (g * sizes[1] + i % sizes[1]) * sizes[2] + j % sizes[2]

    pairs = [
        (place(g, i, j), place(1 - g if across else g, i + lon, j + lat))
        for g in range(sizes[0])
        for i in range(sizes[1])
        for j in range(sizes[2])
    ]
    return lax.ppermute(array, axes, pairs)


def cells_to_tokens(pieces, cells_scr, tokens_scr, row):
    count = 0
    for piece in pieces:
        size = piece.shape[0]
        cells_scr[count * 8 : (count + size) * 8, :] = piece.reshape(size * 8, LANES).astype(
            jnp.float32
        )
        count += size
    for level in range(2):
        for tile in range(4):
            tokens_scr[tile, row + level * count : row + (level + 1) * count, :] = cells_scr[
                pl.ds(2 * tile + level, count, stride=8), :
            ]


def tokens_to_cells(tokens_scr, row, count, cells_scr):
    for level in range(2):
        for tile in range(4):
            cells_scr[pl.ds(2 * tile + level, count, stride=8), :] = tokens_scr[
                tile, row + level * count : row + (level + 1) * count, :
            ]


def whole_rows(tokens_scr):
    return jnp.concatenate([tokens_scr[tile] for tile in range(4)], axis=1)


def layer_norm(values):
    centred = values - jnp.mean(values, -1, keepdims=True)
    return centred * lax.rsqrt(jnp.mean(centred * centred, -1, keepdims=True) + 1e-05)


def head_squares(values, head_size):
    width = 256
    rows = lax.broadcasted_iota(jnp.int32, (width, width), 0) // head_size
    cols = lax.broadcasted_iota(jnp.int32, (width, width), 1) // head_size
    averaging = jnp.where(rows == cols, 1.0 / head_size, 0.0).astype(jnp.bfloat16)
    squares = (values * values).astype(jnp.bfloat16)
    return jnp.concatenate(
        [
            jnp.dot(
                squares[:, at : at + width], averaging, preferred_element_type=jnp.float32
            )
            for at in range(0, values.shape[1], width)
        ],
        axis=1,
    )


def unit_heads(values, head_size):
    return values * lax.rsqrt(head_squares(values, head_size) + 1e-06)


def window_columns(part):
    rows, lanes = [], []
    for source_parts in part:
        for level in range(2):
            for source, lats, lons in source_parts:
                for _ in range(3):
                    for lat in range(*lats):
                        for lon in range(*lons):
                            rows.append(24 * source + 2 * lat + level)
                            lanes.append(lon)
    keys = np.arange(len(rows))
    pick_row = np.zeros((96, len(rows)), np.float32)
    pick_row[np.array(rows), keys] = 1
    pick_lane = np.zeros((16, len(rows)), np.float32)
    pick_lane[np.array(lanes), keys] = 1
    return pick_row, pick_lane


def pack_kernel(cells, mask_hbm, own, west, north, flags, mask, sems):
    copies = []
    mask_copy = pltpu.make_async_copy(mask_hbm, mask, sems.at[1])
    mask_copy.start()
    for g in range(3):
        for dst, first, lats, lons in (
            (west, 0, (3, 9), (0, 6)),
            (west, 108, (9, 12), (0, 6)),
            (west, 162, (0, 3), (0, 6)),
            (own, 0, (3, 9), (6, 12)),
            (own, 108, (9, 12), (6, 12)),
            (north, 0, (0, 3), (6, 12)),
        ):
            rows = lats[1] - lats[0]
            copies.append(
                pltpu.make_async_copy(
                    cells.at[g, lats[0] : lats[1], lons[0] : lons[1]],
                    dst.at[pl.ds(first + g * rows * 6, rows * 6)].reshape(rows, 6, 8, LANES),
                    sems.at[0],
                )
            )
    for copy in copies:
        copy.start()
    flags[...] = jnp.zeros(flags.shape, jnp.float32)
    mask_copy.wait()
    for lat in range(12):
        flags[2 * lat : 2 * lat + 2, 0:12] = mask[lat].astype(jnp.float32)
    tile = flags[...].astype(jnp.bfloat16).reshape(3, 8, LANES)
    west[216:219] = tile
    north[54:57] = tile
    for copy in copies:
        copy.wait()


def again_kernel(east, out):
    out[...] = east[0:162]


def southward_kernel(east, north, after, out):
    out[0:54] = north[0:54]
    out[54:108] = east[162:216]
    out[108:111] = north[54:57]
    out[111:114] = east[216:219]


def attend(query_ref, key_ref, value_ref, bias_ref, head_size, store):
    half = query_ref.shape[0]
    lane = lax.broadcasted_iota(jnp.int32, (half, LANES), 1)

    def one(pair, carry):
        at = pl.multiple_of(pair * LANES, LANES)
        queries = query_ref[:, pl.ds(at, LANES)]
        keys = key_ref[:, pl.ds(at, LANES)]
        values = value_ref[:, pl.ds(at, LANES)]
        total = None
        for side in range(2):
            mine = (lane < head_size) if side == 0 else (lane >= head_size)
            scores = lax.dot_general(
                queries,
                jnp.where(mine, keys, jnp.zeros_like(keys)),
                (((1,), (1,)), ((), ())),
                preferred_element_type=jnp.float32,
            )
            first = bias_ref[pl.ds(2 * pair + side, 1), :]
            second = bias_ref[pl.ds(8 + 2 * pair + side, 1), :]
            scores = jnp.concatenate(
                [scores[: half // 2] + first, scores[half // 2 :] + second], 0
            )
            weights = jnp.exp2(scores).astype(jnp.bfloat16)
            operand = jnp.concatenate(
                [
                    jnp.where(mine, values, jnp.zeros_like(values)),
                    jnp.where(mine, 1.0, 0.0).astype(jnp.bfloat16),
                ],
                axis=1,
            )
            part = jnp.dot(weights, operand, preferred_element_type=jnp.float32)
            total = part if total is None else total + part
        store(pair, at, total)
        return carry

    [one(p, 0) for p in range(4)]


def gather(window, own, east, south, cells_scr, tokens_scr):
    if window == 0:
        cells_to_tokens([own[0:108]], cells_scr, tokens_scr, 0)
        cells_to_tokens([east[0:108]], cells_scr, tokens_scr, 216)
    else:
        cells_to_tokens([own[108:162], east[108:162]], cells_scr, tokens_scr, 0)
        cells_to_tokens([south[0:108]], cells_scr, tokens_scr, 216)


def project(normed, w_qkv, logit_scale, head_size):
    width = w_qkv.shape[0]
    head = lax.broadcasted_iota(jnp.int32, (1, width), 1) // head_size
    scale = jnp.zeros((1, width), jnp.float32)
    for i in range(width // head_size):
        scale = jnp.where(head == i, logit_scale[0:1, i : i + 1] * (LOG2E / head_size), scale)
    mixed = jnp.dot(normed, w_qkv[:, :width], preferred_element_type=jnp.float32)
    queries = unit_heads(mixed, head_size) * scale
    mixed = jnp.dot(normed, w_qkv[:, width : 2 * width], preferred_element_type=jnp.float32)
    keys = unit_heads(mixed, head_size)
    values = jnp.dot(normed, w_qkv[:, 2 * width :], preferred_element_type=jnp.float32)
    return queries, keys, values


def early_kernel(head_size, own, w_qkv, logit_scale, out, cells_scr, tokens_scr):
    cells_to_tokens([own[0:108]], cells_scr, tokens_scr, 0)
    normed = layer_norm(whole_rows(tokens_scr)).astype(jnp.bfloat16)
    for i, part in enumerate(project(normed, w_qkv, logit_scale, head_size)):
        out[i] = part


def own_kernel(
    head_size,
    window,
    own,
    east,
    south,
    after,
    north,
    w_qkv,
    logit_scale,
    mask_bias,
    pick_row,
    pick_lane,
    query_out,
    total_out,
    bias_out,
    cells_scr,
    tokens_scr,
    key_scr,
    value_scr,
):
    if window == 0:
        cells_to_tokens([east[0:108]], cells_scr, tokens_scr, 216)
    else:
        gather(window, own, east, south, cells_scr, tokens_scr)
    marks = [north[54:57], east[216:219]]
    if window == 1:
        marks += [south[108:111], south[111:114]]
    marks = jnp.concatenate([m.reshape(24, LANES).astype(jnp.float32) for m in marks], 0)
    spread = lax.dot_general(
        marks,
        pick_row[0 : marks.shape[0], :],
        (((0,), (0,)), ((), ())),
        preferred_element_type=jnp.float32,
    )
    marks = jnp.sum(spread[0:16] * pick_lane[...], 0, keepdims=True)
    heads = mask_bias.shape[1]
    rows = lax.broadcasted_iota(jnp.int32, (heads, heads), 0)
    cols = lax.broadcasted_iota(jnp.int32, (heads, heads), 1)
    column = jnp.sum(jnp.where(rows == cols, mask_bias[...], 0.0), 1, keepdims=True)
    bias = (column * LOG2E) * marks
    bias_out[0:8, :] = bias
    bias_out[8:16, :] = bias
    if window == 1:
        keys = marks.shape[1]
        later = lax.broadcasted_iota(jnp.int32, (8, keys), 1) >= keys // 2
        last = lax.axis_index("lat") == lax.axis_size("lat") - 1
        excluded = jnp.where(last, EXCLUDED, 0.0)
        bias_out[0:8, :] = bias + jnp.where(later, excluded, 0.0)
        bias_out[8:16, :] = bias + jnp.where(later, 0.0, excluded)
    tokens = whole_rows(tokens_scr)
    if window == 0:
        half = tokens.shape[0] // 2
        normed = layer_norm(tokens[half:]).astype(jnp.bfloat16)
        parts = project(normed, w_qkv, logit_scale, head_size)
        parts = [jnp.concatenate([south[i], part], 0) for i, part in enumerate(parts)]
    else:
        normed = layer_norm(tokens).astype(jnp.bfloat16)
        parts = project(normed, w_qkv, logit_scale, head_size)
    for ref, part in zip((query_out, key_scr, value_scr), parts):
        ref[...] = part.astype(jnp.bfloat16)

    def store(pair, at, total):
        total_out[pair] = total

    attend(query_out, key_scr, value_scr, bias_out, head_size, store)


def partner_kernel(
    head_size,
    window,
    own,
    east,
    south,
    query_ref,
    total_in,
    bias_ref,
    w_qkv,
    w_out,
    *rest,
):
    outs, (cells_scr, tokens_scr, key_scr, value_scr, attended_scr) = rest[:-5], rest[-5:]
    if window == 1:
        upper_east, outs = outs[0], outs[1:]
    gather(window, own, east, south, cells_scr, tokens_scr)
    width = w_qkv.shape[0]
    normed = layer_norm(whole_rows(tokens_scr)).astype(jnp.bfloat16)
    mixed = jnp.dot(normed, w_qkv[:, width : 2 * width], preferred_element_type=jnp.float32)
    key_scr[...] = unit_heads(mixed, head_size).astype(jnp.bfloat16)
    value_scr[...] = jnp.dot(
        normed, w_qkv[:, 2 * width :], preferred_element_type=jnp.float32
    ).astype(jnp.bfloat16)

    def store(pair, at, total):
        total = total + total_in[pair]
        attended_scr[:, pl.ds(at, LANES)] = (total[:, :LANES] / total[:, LANES:]).astype(
            jnp.bfloat16
        )

    attend(query_ref, key_scr, value_scr, bias_ref, head_size, store)
    projected = jnp.dot(attended_scr[...], w_out[...], preferred_element_type=jnp.float32)
    for tile in range(4):
        tokens_scr[tile] = projected[:, tile * LANES : (tile + 1) * LANES]

    def put(row, count, outs):
        tokens_to_cells(tokens_scr, row, count, cells_scr)
        at = 0
        for out, size in outs:
            out[...] = (
                cells_scr[at * 8 : (at + size) * 8, :].astype(jnp.bfloat16).reshape(size, 8, LANES)
            )
            at += size

    if window == 0:
        put(0, 108, [(outs[0], 108)])
        put(216, 108, [(outs[1], 108)])
    else:
        put(0, 108, [(outs[0], 54), (outs[1].at[0:54], 54)])
        put(216, 108, [(outs[2], 54), (outs[3], 54)])
        outs[1][54:162] = upper_east[...]


def joining_kernel(bands, batches, fields, w_up, w_down, *rest):
    pieces, rest = rest[: 2 * len(bands)], rest[2 * len(bands) :]
    copies = []
    if len(bands) == 2:
        out, cells_scr, tokens_scr = rest
    else:
        done, out, cells_scr, tokens_scr, rounded, sems = rest
        copies.append(pltpu.make_async_copy(done, out.at[:, 3:12], sems.at[0]))
        copies[0].start()
    for batch, (start, stop) in enumerate(batches):
        for g in range(start, stop):
            at = 0
            for band, (first, rows, skips) in enumerate(bands):
                for side, lons in enumerate(((6, 12), (0, 6))):
                    size = rows * 6
                    begin = skips[side] + g * size
                    term = pieces[2 * band + side][begin : begin + size].astype(jnp.float32)
                    term = term.reshape(rows, 6, 8, LANES)
                    summed = fields[g, first : first + rows, lons[0] : lons[1]]
                    summed = (summed.astype(jnp.float32) + term).astype(jnp.bfloat16)
                    cells_scr[g, at : at + rows, lons[0] : lons[1]] = summed.astype(jnp.float32)
                at += rows
        cells = (stop - start) * at * 12
        flat = cells_scr.at[start:stop].reshape(cells * 8, LANES)
        for level in range(2):
            for tile in range(4):
                tokens_scr[
                    batch, level * cells : (level + 1) * cells, tile * LANES : (tile + 1) * LANES
                ] = flat[pl.ds(2 * tile + level, cells, stride=8), :]
        residual = tokens_scr[batch]
        normed = layer_norm(residual).astype(jnp.bfloat16)
        hidden = jnp.dot(normed, w_up[...], preferred_element_type=jnp.float32)
        hidden = jax.nn.gelu(hidden, approximate=True).astype(jnp.bfloat16)
        tokens_scr[batch] = residual + jnp.dot(
            hidden, w_down[...], preferred_element_type=jnp.float32
        )
        for level in range(2):
            for tile in range(4):
                flat[pl.ds(2 * tile + level, cells, stride=8), :] = tokens_scr[
                    batch, level * cells : (level + 1) * cells, tile * LANES : (tile + 1) * LANES
                ]
        if len(bands) == 2:
            out[start:stop] = cells_scr[start:stop].astype(jnp.bfloat16)
    if len(bands) == 1:
        rounded[...] = cells_scr[...].astype(jnp.bfloat16)
        copies.append(pltpu.make_async_copy(rounded, out.at[:, 0:3], sems.at[1]))
        copies[1].start()
    for copy in copies:
        copy.wait()


def per_device(fields, surface_mask, w_qkv, w_out, logit_scale, mask_bias, w_up, w_down):
    groups, levels, lat_rows, lon_cells, width = fields.shape
    heads = logit_scale.shape[0]
    head_size = width // heads
    half = groups * levels * lat_rows * lon_cells // 2
    cells = to_pairs(fields)
    tile = (8, LANES)

    def pieces(*counts):
        return tuple(jax.ShapeDtypeStruct((n,) + tile, jnp.bfloat16) for n in counts)

    def call(kernel, outs, scratch, flops, arrays, space=VMEM):
        return pl.pallas_call(
            kernel,
            compiler_params=ROOM,
            out_shape=outs,
            in_specs=[VMEM] * len(arrays),
            out_specs=jax.tree.map(lambda _: space, outs),
            scratch_shapes=scratch,
            cost_estimate=pl.CostEstimate(
                flops=flops, bytes_accessed=4 * 10**6, transcendentals=10**6
            ),
        )(*arrays)

    own, west, north = pl.pallas_call(
        pack_kernel,
        name="pack",
        compiler_params=ROOM,
        out_shape=pieces(162, 219, 57),
        in_specs=[pl.BlockSpec(memory_space=pltpu.HBM)] * 2,
        out_specs=(VMEM, VMEM, VMEM),
        scratch_shapes=[
            pltpu.VMEM((24, LANES), jnp.float32),
            pltpu.VMEM((lat_rows, levels, lon_cells), jnp.int32),
            pltpu.SemaphoreType.DMA((2,)),
        ],
    )(
        pltpu.with_memory_space_constraint(cells, pltpu.HBM),
        pltpu.with_memory_space_constraint(jnp.transpose(surface_mask, (1, 0, 2)), pltpu.HBM),
    )
    east = shifted(west, lon=-1)
    own_across = shifted(own, across=True)
    east_again = call(again_kernel, pieces(162)[0], [], 10**6, (east,))
    east_across = shifted(east_again, across=True)

    layout = (
        (((0, (3, 9), (6, 12)),), ((1, (3, 9), (0, 6)),)),
        (((0, (9, 12), (6, 12)), (1, (9, 12), (0, 6))), ((2, (0, 3), (6, 12)), (3, (0, 3), (0, 6)))),
    )
    scratch = [
        pltpu.VMEM((half * 2, LANES), jnp.float32),
        pltpu.VMEM((4, half, LANES), jnp.float32),
        pltpu.VMEM((half, width), jnp.bfloat16),
        pltpu.VMEM((half, width), jnp.bfloat16),
    ]
    late = scratch + [pltpu.VMEM((half, width), jnp.bfloat16)]

    def own_part(window, arrays):
        pick_row, pick_lane = window_columns(layout[window])
        return call(
            functools.partial(own_kernel, head_size, window),
            (
                jax.ShapeDtypeStruct((half, width), jnp.bfloat16),
                jax.ShapeDtypeStruct((4, half, 2 * LANES), jnp.float32),
                jax.ShapeDtypeStruct((16, half), jnp.float32),
            ),
            scratch,
            3 * 10**9,
            arrays + (w_qkv, logit_scale[None], mask_bias[None], pick_row, pick_lane),
        )

    def partner_part(window, counts, arrays, first, more):
        return call(
            functools.partial(partner_kernel, head_size, window),
            pieces(*counts),
            late,
            3 * 10**9,
            arrays + tuple(first) + (w_qkv, w_out) + more,
        )

    early = call(
        functools.partial(early_kernel, head_size),
        jax.ShapeDtypeStruct((3, half // 2, width), jnp.float32),
        [
            pltpu.VMEM((half * 2, LANES), jnp.float32),
            pltpu.VMEM((4, half // 2, LANES), jnp.float32),
        ],
        3 * 10**8,
        (own, w_qkv, logit_scale[None]),
    )
    first = own_part(0, (own, east, early, north, north))
    south = call(southward_kernel, pieces(114)[0], [], 10**6, (east, north, first[2]))
    south_across = shifted(south, lat=-1, across=True)
    south = shifted(south, lat=-1)
    upper_own, upper_east = partner_part(
        0, (108, 108), (own_across, east_across, own_across), first, ()
    )
    first = own_part(1, (own, east, south, upper_own, north))
    lower_own, all_east, lower_south, lower_corner = partner_part(
        1, (54, 162, 54, 54), (own_across, east_across, south_across), first, (upper_east,)
    )
    west = shifted(all_east, lon=1)
    lower_northwest = shifted(lower_corner, lon=1, lat=1)
    lower_north = shifted(lower_south, lat=1)
    rest = (groups, lat_rows - SH_LAT, lon_cells) + tile
    edge = (groups, SH_LAT, lon_cells) + tile
    upper = call(
        functools.partial(
            joining_kernel,
            ((3, 6, (0, 54)), (9, 3, (0, 0))),
            [(g, g + 1) for g in range(groups)],
        ),
        jax.ShapeDtypeStruct(rest, jnp.bfloat16),
        [
            pltpu.VMEM(rest, jnp.float32),
            pltpu.VMEM((groups, half // 2, width), jnp.float32),
        ],
        3 * 10**9,
        (cells, w_up, w_down, upper_own, west, lower_own, west),
    )
    joined = call(
        functools.partial(joining_kernel, ((0, 3, (0, 0)),), [(0, groups)]),
        jax.ShapeDtypeStruct(cells.shape, jnp.bfloat16),
        [
            pltpu.VMEM(edge, jnp.float32),
            pltpu.VMEM((1, half // 2, width), jnp.float32),
            pltpu.VMEM(edge, jnp.bfloat16),
            pltpu.SemaphoreType.DMA((2,)),
        ],
        10**9,
        (cells, w_up, w_down, lower_north, lower_northwest, upper),
        pl.BlockSpec(memory_space=pltpu.HBM),
    )
    return from_pairs(joined, levels)


def solution(mesh):
    return jax.shard_map(
        per_device,
        mesh=mesh,
        in_specs=(
            P("grp", None, "lat", "lon", None),
            P(None, "lat", "lon"),
            P(),
            P(),
            P(),
            P(),
            P(),
            P(),
        ),
        out_specs=P("grp", None, "lat", "lon", None),
        check_vma=False,
    )
```

```python
import functools

import jax
import jax.numpy as jnp
import numpy as np
from jax import lax
from jax.experimental import pallas as pl
from jax.experimental.pallas import tpu as pltpu
from jax.sharding import PartitionSpec as P


LANES = 128
SH_LAT = 3
LOG2E = 1.4426950408889634
EXCLUDED = -1e30
VMEM = pl.BlockSpec(memory_space=pltpu.VMEM)
SMEM = pl.BlockSpec(memory_space=pltpu.SMEM)
ROOM = pltpu.CompilerParams(vmem_limit_bytes=24 << 20)


def to_pairs(fields):
    groups, levels, lat_rows, lon_cells, width = fields.shape
    cells = jnp.transpose(fields, (0, 2, 3, 1, 4))
    cells = cells.reshape(groups, lat_rows, lon_cells, levels, width // LANES, LANES)
    cells = jnp.transpose(cells, (0, 1, 2, 4, 3, 5))
    return cells.reshape(groups, lat_rows, lon_cells, levels * (width // LANES), LANES)


def from_pairs(cells, levels):
    groups, lat_rows, lon_cells, rows, lanes = cells.shape
    cells = cells.reshape(groups, lat_rows, lon_cells, rows // levels, levels, lanes)
    cells = jnp.transpose(cells, (0, 1, 2, 4, 3, 5))
    cells = cells.reshape(groups, lat_rows, lon_cells, levels, (rows // levels) * lanes)
    return jnp.transpose(cells, (0, 3, 1, 2, 4))


def shifted(array, lon=0, lat=0, across=False):
    axes = ("grp", "lon", "lat")
    sizes = [lax.axis_size(axis) for axis in axes]

    def place(g, i, j):
        return (g * sizes[1] + i % sizes[1]) * sizes[2] + j % sizes[2]

    pairs = [
        (place(g, i, j), place(1 - g if across else g, i + lon, j + lat))
        for g in range(sizes[0])
        for i in range(sizes[1])
        for j in range(sizes[2])
    ]
    return lax.ppermute(array, axes, pairs)


def cells_to_tokens(pieces, cells_scr, tokens_scr, row):
    count = 0
    for piece in pieces:
        size = piece.shape[0]
        cells_scr[count * 8 : (count + size) * 8, :] = piece.reshape(size * 8, LANES).astype(
            jnp.float32
        )
        count += size
    for level in range(2):
        for tile in range(4):
            tokens_scr[tile, row + level * count : row + (level + 1) * count, :] = cells_scr[
                pl.ds(2 * tile + level, count, stride=8), :
            ]


def tokens_to_cells(tokens_scr, row, count, cells_scr):
    for level in range(2):
        for tile in range(4):
            cells_scr[pl.ds(2 * tile + level, count, stride=8), :] = tokens_scr[
                tile, row + level * count : row + (level + 1) * count, :
            ]


def whole_rows(tokens_scr):
    return jnp.concatenate([tokens_scr[tile] for tile in range(4)], axis=1)


def layer_norm(values):
    centred = values - jnp.mean(values, -1, keepdims=True)
    return centred * lax.rsqrt(jnp.mean(centred * centred, -1, keepdims=True) + 1e-05)


def unit_heads(values, head_size):
    lane = lax.broadcasted_iota(jnp.int32, (1, LANES), 1)
    parts = []
    for at in range(0, values.shape[1], LANES):
        part = values[:, at : at + LANES]
        squares = part * part
        left = jnp.sum(jnp.where(lane < head_size, squares, 0.0), 1, keepdims=True)
        right = jnp.sum(jnp.where(lane < head_size, 0.0, squares), 1, keepdims=True)
        mean = jnp.where(lane < head_size, left, right) * (1.0 / head_size)
        parts.append(part * lax.rsqrt(mean + 1e-06))
    return jnp.concatenate(parts, axis=1)


def window_columns(part):
    rows, lanes = [], []
    for source_parts in part:
        for level in range(2):
            for source, lats, lons in source_parts:
                for _ in range(3):
                    for lat in range(*lats):
                        for lon in range(*lons):
                            rows.append(24 * source + 2 * lat + level)
                            lanes.append(lon)
    keys = np.arange(len(rows))
    pick_row = np.zeros((96, len(rows)), np.float32)
    pick_row[np.array(rows), keys] = 1
    pick_lane = np.zeros((16, len(rows)), np.float32)
    pick_lane[np.array(lanes), keys] = 1
    return pick_row, pick_lane


def pack_kernel(cells, mask_hbm, own, west, north, flags, mask, sems):
    copies = []
    mask_copy = pltpu.make_async_copy(mask_hbm, mask, sems.at[1])
    mask_copy.start()
    for g in range(3):
        for dst, first, lats, lons in (
            (west, 0, (3, 9), (0, 6)),
            (west, 108, (9, 12), (0, 6)),
            (west, 162, (0, 3), (0, 6)),
            (own, 0, (3, 9), (6, 12)),
            (own, 108, (9, 12), (6, 12)),
            (north, 0, (0, 3), (6, 12)),
        ):
            rows = lats[1] - lats[0]
            copies.append(
                pltpu.make_async_copy(
                    cells.at[g, lats[0] : lats[1], lons[0] : lons[1]],
                    dst.at[pl.ds(first + g * rows * 6, rows * 6)].reshape(rows, 6, 8, LANES),
                    sems.at[0],
                )
            )
    for copy in copies:
        copy.start()
    flags[...] = jnp.zeros(flags.shape, jnp.float32)
    mask_copy.wait()
    for lat in range(12):
        flags[2 * lat : 2 * lat + 2, 0:12] = mask[lat].astype(jnp.float32)
    tile = flags[...].astype(jnp.bfloat16).reshape(3, 8, LANES)
    west[216:219] = tile
    north[54:57] = tile
    for copy in copies:
        copy.wait()


def again_kernel(east, out):
    out[...] = east[0:162]


def southward_kernel(east, north, after, out):
    out[0:54] = north[0:54]
    out[54:108] = east[162:216]
    out[108:111] = north[54:57]
    out[111:114] = east[216:219]


def attend(query_ref, key_ref, value_ref, bias_ref, head_size, store):
    half = query_ref.shape[0]
    lane = lax.broadcasted_iota(jnp.int32, (half, LANES), 1)

    def one(pair, carry):
        at = pl.multiple_of(pair * LANES, LANES)
        queries = query_ref[:, pl.ds(at, LANES)]
        keys = key_ref[:, pl.ds(at, LANES)]
        values = value_ref[:, pl.ds(at, LANES)]
        total = None
        for side in range(2):
            mine = (lane < head_size) if side == 0 else (lane >= head_size)
            scores = lax.dot_general(
                queries,
                jnp.where(mine, keys, jnp.zeros_like(keys)),
                (((1,), (1,)), ((), ())),
                preferred_element_type=jnp.float32,
            )
            first = bias_ref[pl.ds(2 * pair + side, 1), :]
            second = bias_ref[pl.ds(8 + 2 * pair + side, 1), :]
            scores = jnp.concatenate(
                [scores[: half // 2] + first, scores[half // 2 :] + second], 0
            )
            weights = jnp.exp2(scores).astype(jnp.bfloat16)
            operand = jnp.concatenate(
                [
                    jnp.where(mine, values, jnp.zeros_like(values)),
                    jnp.where(mine, 1.0, 0.0).astype(jnp.bfloat16),
                ],
                axis=1,
            )
            part = jnp.dot(weights, operand, preferred_element_type=jnp.float32)
            total = part if total is None else total + part
        store(pair, at, total)
        return carry

    [one(p, 0) for p in range(4)]


def gather(window, own, east, south, cells_scr, tokens_scr):
    if window == 0:
        cells_to_tokens([own[0:108]], cells_scr, tokens_scr, 0)
        cells_to_tokens([east[0:108]], cells_scr, tokens_scr, 216)
    else:
        cells_to_tokens([own[108:162], east[108:162]], cells_scr, tokens_scr, 0)
        cells_to_tokens([south[0:108]], cells_scr, tokens_scr, 216)


def project(normed, w_qkv, logit_scale, head_size):
    width = w_qkv.shape[0]
    head = lax.broadcasted_iota(jnp.int32, (1, width), 1) // head_size
    scale = jnp.zeros((1, width), jnp.float32)
    for i in range(width // head_size):
        scale = jnp.where(head == i, logit_scale[0:1, i : i + 1] * (LOG2E / head_size), scale)
    mixed = jnp.dot(normed, w_qkv[:, :width], preferred_element_type=jnp.float32)
    queries = unit_heads(mixed, head_size) * scale
    mixed = jnp.dot(normed, w_qkv[:, width : 2 * width], preferred_element_type=jnp.float32)
    keys = unit_heads(mixed, head_size)
    values = jnp.dot(normed, w_qkv[:, 2 * width :], preferred_element_type=jnp.float32)
    return queries, keys, values


def early_kernel(head_size, own, w_qkv, logit_scale, out, cells_scr, tokens_scr):
    cells_to_tokens([own[0:108]], cells_scr, tokens_scr, 0)
    normed = layer_norm(whole_rows(tokens_scr)).astype(jnp.bfloat16)
    for i, part in enumerate(project(normed, w_qkv, logit_scale, head_size)):
        out[i] = part


def own_kernel(
    head_size,
    window,
    own,
    east,
    south,
    after,
    north,
    w_qkv,
    logit_scale,
    mask_bias,
    pick_row,
    pick_lane,
    query_out,
    total_out,
    bias_out,
    cells_scr,
    tokens_scr,
    key_scr,
    value_scr,
):
    if window == 0:
        cells_to_tokens([east[0:108]], cells_scr, tokens_scr, 216)
    else:
        gather(window, own, east, south, cells_scr, tokens_scr)
    marks = [north[54:57], east[216:219]]
    if window == 1:
        marks += [south[108:111], south[111:114]]
    marks = jnp.concatenate([m.reshape(24, LANES).astype(jnp.float32) for m in marks], 0)
    spread = lax.dot_general(
        marks,
        pick_row[0 : marks.shape[0], :],
        (((0,), (0,)), ((), ())),
        preferred_element_type=jnp.float32,
    )
    marks = jnp.sum(spread[0:16] * pick_lane[...], 0, keepdims=True)
    heads = mask_bias.shape[1]
    rows = lax.broadcasted_iota(jnp.int32, (heads, heads), 0)
    cols = lax.broadcasted_iota(jnp.int32, (heads, heads), 1)
    column = jnp.sum(jnp.where(rows == cols, mask_bias[...], 0.0), 1, keepdims=True)
    bias = (column * LOG2E) * marks
    bias_out[0:8, :] = bias
    bias_out[8:16, :] = bias
    if window == 1:
        keys = marks.shape[1]
        later = lax.broadcasted_iota(jnp.int32, (8, keys), 1) >= keys // 2
        last = lax.axis_index("lat") == lax.axis_size("lat") - 1
        excluded = jnp.where(last, EXCLUDED, 0.0)
        bias_out[0:8, :] = bias + jnp.where(later, excluded, 0.0)
        bias_out[8:16, :] = bias + jnp.where(later, 0.0, excluded)
    tokens = whole_rows(tokens_scr)
    if window == 0:
        half = tokens.shape[0] // 2
        normed = layer_norm(tokens[half:]).astype(jnp.bfloat16)
        parts = project(normed, w_qkv, logit_scale, head_size)
        parts = [jnp.concatenate([south[i], part], 0) for i, part in enumerate(parts)]
    else:
        normed = layer_norm(tokens).astype(jnp.bfloat16)
        parts = project(normed, w_qkv, logit_scale, head_size)
    for ref, part in zip((query_out, key_scr, value_scr), parts):
        ref[...] = part.astype(jnp.bfloat16)

    def store(pair, at, total):
        total_out[pair] = total

    attend(query_out, key_scr, value_scr, bias_out, head_size, store)


def partner_kernel(
    head_size,
    window,
    own,
    east,
    south,
    query_ref,
    total_in,
    bias_ref,
    w_qkv,
    w_out,
    *rest,
):
    outs, (cells_scr, tokens_scr, key_scr, value_scr, attended_scr) = rest[:-5], rest[-5:]
    if window == 1:
        upper_east, outs = outs[0], outs[1:]
    gather(window, own, east, south, cells_scr, tokens_scr)
    width = w_qkv.shape[0]
    normed = layer_norm(whole_rows(tokens_scr)).astype(jnp.bfloat16)
    mixed = jnp.dot(normed, w_qkv[:, width : 2 * width], preferred_element_type=jnp.float32)
    key_scr[...] = unit_heads(mixed, head_size).astype(jnp.bfloat16)
    value_scr[...] = jnp.dot(
        normed, w_qkv[:, 2 * width :], preferred_element_type=jnp.float32
    ).astype(jnp.bfloat16)

    def store(pair, at, total):
        total = total + total_in[pair]
        attended_scr[:, pl.ds(at, LANES)] = (total[:, :LANES] / total[:, LANES:]).astype(
            jnp.bfloat16
        )

    attend(query_ref, key_scr, value_scr, bias_ref, head_size, store)
    projected = jnp.dot(attended_scr[...], w_out[...], preferred_element_type=jnp.float32)
    for tile in range(4):
        tokens_scr[tile] = projected[:, tile * LANES : (tile + 1) * LANES]

    def put(row, count, outs):
        tokens_to_cells(tokens_scr, row, count, cells_scr)
        at = 0
        for out, size in outs:
            out[...] = (
                cells_scr[at * 8 : (at + size) * 8, :].astype(jnp.bfloat16).reshape(size, 8, LANES)
            )
            at += size

    if window == 0:
        put(0, 108, [(outs[0], 108)])
        put(216, 108, [(outs[1], 108)])
    else:
        put(0, 108, [(outs[0], 54), (outs[1].at[0:54], 54)])
        put(216, 108, [(outs[2], 54), (outs[3], 54)])
        outs[1][54:162] = upper_east[...]


def joining_kernel(bands, batches, fields, w_up, w_down, *rest):
    pieces, rest = rest[: 2 * len(bands)], rest[2 * len(bands) :]
    copies = []
    if len(bands) == 2:
        out, cells_scr, tokens_scr = rest
    else:
        done, out, cells_scr, tokens_scr, rounded, sems = rest
        copies.append(pltpu.make_async_copy(done, out.at[:, 3:12], sems.at[0]))
        copies[0].start()
    for batch, (start, stop) in enumerate(batches):
        for g in range(start, stop):
            at = 0
            for band, (first, rows, skips) in enumerate(bands):
                for side, lons in enumerate(((6, 12), (0, 6))):
                    size = rows * 6
                    begin = skips[side] + g * size
                    term = pieces[2 * band + side][begin : begin + size].astype(jnp.float32)
                    term = term.reshape(rows, 6, 8, LANES)
                    summed = fields[g, first : first + rows, lons[0] : lons[1]]
                    summed = (summed.astype(jnp.float32) + term).astype(jnp.bfloat16)
                    cells_scr[g, at : at + rows, lons[0] : lons[1]] = summed.astype(jnp.float32)
                at += rows
        cells = (stop - start) * at * 12
        flat = cells_scr.at[start:stop].reshape(cells * 8, LANES)
        for level in range(2):
            for tile in range(4):
                tokens_scr[
                    batch, level * cells : (level + 1) * cells, tile * LANES : (tile + 1) * LANES
                ] = flat[pl.ds(2 * tile + level, cells, stride=8), :]
        residual = tokens_scr[batch]
        normed = layer_norm(residual).astype(jnp.bfloat16)
        hidden = jnp.dot(normed, w_up[...], preferred_element_type=jnp.float32)
        hidden = jax.nn.gelu(hidden, approximate=True).astype(jnp.bfloat16)
        tokens_scr[batch] = residual + jnp.dot(
            hidden, w_down[...], preferred_element_type=jnp.float32
        )
        for level in range(2):
            for tile in range(4):
                flat[pl.ds(2 * tile + level, cells, stride=8), :] = tokens_scr[
                    batch, level * cells : (level + 1) * cells, tile * LANES : (tile + 1) * LANES
                ]
        if len(bands) == 2:
            out[start:stop] = cells_scr[start:stop].astype(jnp.bfloat16)
    if len(bands) == 1:
        rounded[...] = cells_scr[...].astype(jnp.bfloat16)
        copies.append(pltpu.make_async_copy(rounded, out.at[:, 0:3], sems.at[1]))
        copies[1].start()
    for copy in copies:
        copy.wait()


def per_device(fields, surface_mask, w_qkv, w_out, logit_scale, mask_bias, w_up, w_down):
    groups, levels, lat_rows, lon_cells, width = fields.shape
    heads = logit_scale.shape[0]
    head_size = width // heads
    half = groups * levels * lat_rows * lon_cells // 2
    cells = to_pairs(fields)
    tile = (8, LANES)

    def pieces(*counts):
        return tuple(jax.ShapeDtypeStruct((n,) + tile, jnp.bfloat16) for n in counts)

    def call(kernel, outs, scratch, flops, arrays, space=VMEM):
        return pl.pallas_call(
            kernel,
            compiler_params=ROOM,
            out_shape=outs,
            in_specs=[VMEM] * len(arrays),
            out_specs=jax.tree.map(lambda _: space, outs),
            scratch_shapes=scratch,
            cost_estimate=pl.CostEstimate(
                flops=flops, bytes_accessed=4 * 10**6, transcendentals=10**6
            ),
        )(*arrays)

    own, west, north = pl.pallas_call(
        pack_kernel,
        name="pack",
        compiler_params=ROOM,
        out_shape=pieces(162, 219, 57),
        in_specs=[pl.BlockSpec(memory_space=pltpu.HBM)] * 2,
        out_specs=(VMEM, VMEM, VMEM),
        scratch_shapes=[
            pltpu.VMEM((24, LANES), jnp.float32),
            pltpu.VMEM((lat_rows, levels, lon_cells), jnp.int32),
            pltpu.SemaphoreType.DMA((2,)),
        ],
    )(
        pltpu.with_memory_space_constraint(cells, pltpu.HBM),
        pltpu.with_memory_space_constraint(jnp.transpose(surface_mask, (1, 0, 2)), pltpu.HBM),
    )
    east = shifted(west, lon=-1)
    own_across = shifted(own, across=True)
    east_again = call(again_kernel, pieces(162)[0], [], 10**6, (east,))
    east_across = shifted(east_again, across=True)

    layout = (
        (((0, (3, 9), (6, 12)),), ((1, (3, 9), (0, 6)),)),
        (((0, (9, 12), (6, 12)), (1, (9, 12), (0, 6))), ((2, (0, 3), (6, 12)), (3, (0, 3), (0, 6)))),
    )
    scratch = [
        pltpu.VMEM((half * 2, LANES), jnp.float32),
        pltpu.VMEM((4, half, LANES), jnp.float32),
        pltpu.VMEM((half, width), jnp.bfloat16),
        pltpu.VMEM((half, width), jnp.bfloat16),
    ]
    late = scratch + [pltpu.VMEM((half, width), jnp.bfloat16)]

    def own_part(window, arrays):
        pick_row, pick_lane = window_columns(layout[window])
        return call(
            functools.partial(own_kernel, head_size, window),
            (
                jax.ShapeDtypeStruct((half, width), jnp.bfloat16),
                jax.ShapeDtypeStruct((4, half, 2 * LANES), jnp.float32),
                jax.ShapeDtypeStruct((16, half), jnp.float32),
            ),
            scratch,
            3 * 10**9,
            arrays + (w_qkv, logit_scale[None], mask_bias[None], pick_row, pick_lane),
        )

    def partner_part(window, counts, arrays, first, more):
        return call(
            functools.partial(partner_kernel, head_size, window),
            pieces(*counts),
            late,
            3 * 10**9,
            arrays + tuple(first) + (w_qkv, w_out) + more,
        )

    early = call(
        functools.partial(early_kernel, head_size),
        jax.ShapeDtypeStruct((3, half // 2, width), jnp.float32),
        [
            pltpu.VMEM((half * 2, LANES), jnp.float32),
            pltpu.VMEM((4, half // 2, LANES), jnp.float32),
        ],
        3 * 10**8,
        (own, w_qkv, logit_scale[None]),
    )
    first = own_part(0, (own, east, early, north, north))
    south = call(southward_kernel, pieces(114)[0], [], 10**6, (east, north, first[2]))
    south_across = shifted(south, lat=-1, across=True)
    south = shifted(south, lat=-1)
    upper_own, upper_east = partner_part(
        0, (108, 108), (own_across, east_across, own_across), first, ()
    )
    first = own_part(1, (own, east, south, upper_own, north))
    lower_own, all_east, lower_south, lower_corner = partner_part(
        1, (54, 162, 54, 54), (own_across, east_across, south_across), first, (upper_east,)
    )
    west = shifted(all_east, lon=1)
    lower_northwest = shifted(lower_corner, lon=1, lat=1)
    lower_north = shifted(lower_south, lat=1)
    rest = (groups, lat_rows - SH_LAT, lon_cells) + tile
    edge = (groups, SH_LAT, lon_cells) + tile
    upper = call(
        functools.partial(
            joining_kernel,
            ((3, 6, (0, 54)), (9, 3, (0, 0))),
            [(g, g + 1) for g in range(groups)],
        ),
        jax.ShapeDtypeStruct(rest, jnp.bfloat16),
        [
            pltpu.VMEM(rest, jnp.float32),
            pltpu.VMEM((groups, half // 2, width), jnp.float32),
        ],
        3 * 10**9,
        (cells, w_up, w_down, upper_own, west, lower_own, west),
    )
    joined = call(
        functools.partial(joining_kernel, ((0, 3, (0, 0)),), [(0, groups)]),
        jax.ShapeDtypeStruct(cells.shape, jnp.bfloat16),
        [
            pltpu.VMEM(edge, jnp.float32),
            pltpu.VMEM((1, half // 2, width), jnp.float32),
            pltpu.VMEM(edge, jnp.bfloat16),
            pltpu.SemaphoreType.DMA((2,)),
        ],
        10**9,
        (cells, w_up, w_down, lower_north, lower_northwest, upper),
        pl.BlockSpec(memory_space=pltpu.HBM),
    )
    return from_pairs(joined, levels)


def solution(mesh):
    return jax.shard_map(
        per_device,
        mesh=mesh,
        in_specs=(
            P("grp", None, "lat", "lon", None),
            P(None, "lat", "lon"),
            P(),
            P(),
            P(),
            P(),
            P(),
            P(),
        ),
        out_specs=P("grp", None, "lat", "lon", None),
        check_vma=False,
    )
```
